256 devices in a mesh: hot: 64 (over z, y, x_lo), cold: 4 (over x_hi, core).
Axes of the slice: x: 4 (x_hi: 2, x_lo: 2; x = x_hi * 2 + x_lo), y: 4, z: 8, core: 2. Of those that a mesh axis runs over, the one named last changes fastest.
Arguments:
- tokens: bfloat16 [64, 8192], replicated, may hold values from -6 to 6
- norm_gain: float32 [8192], replicated, may hold values from 0.1 to 1.9
- hot_gate: bfloat16 [4096, 8192], P(('hot', 'cold')), may hold values from -0.0625 to 0.0625
- hot_up: bfloat16 [4096, 8192], P(('hot', 'cold')), may hold values from -0.0625 to 0.0625
- hot_down: bfloat16 [4096, 8192], P(('hot', 'cold')), may hold values from -0.21875 to 0.21875
- hot_index: int32 [4096], replicated, may hold values from 0 to 14335, as said below
- cold_gate: bfloat16 [8192, 14336], P('hot', 'cold'), may hold values from -0.0625 to 0.0625
- cold_up: bfloat16 [8192, 14336], P('hot', 'cold'), may hold values from -0.0625 to 0.0625
- cold_down: bfloat16 [14336, 8192], P('cold', 'hot'), may hold values from -0.125 to 0.125
- block_mask: int32 [64, 112], P(None, 'cold'), may hold values from 0 to 1, as said below
Outputs:
- ffn_out: bfloat16 [64, 8192], P(None, ('hot', 'cold'))
The draws below stay inside these ranges and needn't reach their ends.
Inputs may be any that keep to these rules, and one draw needn't show every extreme that they name: `hot_index`: distinct hidden units. `block_mask`: in each run of 28 blocks held by one index of cold, at most 14 blocks are active for any sequence, and some index reaches exactly 14.
All inputs are finite; a program needn't handle non-finite values.
Results may differ from the reference program's by a relative error of at most 0.0065.
Values may be sent and summed in bfloat16 or wider, within the bound.
A program may use at most 64 MiB of HBM per device.

```python
import jax
import jax.numpy as jnp
from jax import lax

D = 8192
UNITS = 14336
BLOCK = 128
SEQ = 64
HOT = 4096
BLOCKS = 112
BLK_DEV = 28
CAP = 14


def draw_hot_index(key, part):
    return jax.random.permutation(jax.random.fold_in(key, 11), UNITS)[:HOT].astype(jnp.int32)


def draw_block_mask(key, part):
    groups = BLOCKS // BLK_DEV
    key_busy, key_count, key_rank, key_bits = jax.random.split(jax.random.fold_in(key, 23), 4)
    busy = jax.random.randint(key_busy, (), 0, groups)
    counts = jax.random.randint(key_count, (groups,), CAP // 8, CAP // 3 + 1)
    counts = jnp.where(jnp.arange(groups) == busy, CAP, counts)
    scores = jax.random.randint(key_rank, (groups, BLK_DEV), 0, 1048576) * BLK_DEV + jnp.arange(BLK_DEV)[None, :]
    ranks = jnp.argsort(jnp.argsort(scores, axis=1), axis=1)
    active = (ranks < counts[:, None]).astype(jnp.int32).reshape(BLOCKS)
    bits = jax.random.randint(key_bits, (SEQ, BLOCKS), 0, 2)
    forced = (jnp.arange(SEQ)[:, None] == (jnp.arange(BLOCKS) % SEQ)[None, :]).astype(jnp.int32)
    return (active[None, :] * jnp.maximum(bits, forced)).astype(jnp.int32)


def strengthened(array, rng, source, target, blocks, factor):
    owner, partner = [(jnp.arange(array.shape[dim]) // (array.shape[dim] // blocks)).reshape([-1 if axis == dim else 1 for axis in range(array.ndim)]) for dim in (source, target)]
    chosen = jax.random.permutation(rng, blocks)[partner]
    strong = (owner == chosen) | (owner == (partner + blocks // 2) % blocks)
    return jnp.where(strong, factor * array, array)


def level_of(stream_key, shape, pieces, least, top_value):
    gain = 1.0
    for position, blocks in pieces:
        draws = jax.random.uniform(jax.random.fold_in(jax.random.fold_in(stream_key, 6), position), (blocks,), jnp.float32, least / len(pieces), top_value / len(pieces))
        gain = gain * jnp.repeat(jnp.exp(draws), shape[position] // blocks).reshape((-1,) + (1,) * (len(shape) - 1 - position))
    return gain


def centred(own_key, shape, deviation, bound, shards=(), dtype=jnp.bfloat16):
    values = jax.random.normal(own_key, shape, jnp.float32) * deviation
    if len(shards) > 0:
        values = level_of(own_key, shape, shards, -0.22, 0.18) * values
    return jnp.clip(values, min=-bound, max=bound).astype(dtype)


def heavy_noise(rng, extent, scale, reach, shards, heavy, kind=jnp.bfloat16):
    entries = scale * jax.random.normal(rng, extent, jnp.float32)
    if shards:
        entries = entries * level_of(rng, extent, shards, -0.22, 0.18)
    return jnp.clip(strengthened(entries, jax.random.fold_in(rng, 3), *heavy), -reach, reach).astype(kind)


def setup_inputs(seed: int = 0) -> dict:
    seeds = jax.random.split(jax.random.key(seed), 11)
    tokens = centred(seeds[0], (SEQ, D), 1.0, 6.0)
    norm_gain = jnp.clip(1.0 + 0.18 * jax.random.normal(seeds[1], (D,), jnp.float32), 0.1, 1.9)
    hot_gate = centred(seeds[2], (HOT, D), D ** -0.5, 0.0625, ((0, 256),))
    hot_up = centred(seeds[3], (HOT, D), D ** -0.5, 0.0625, ((0, 256),))
    hot_down = heavy_noise(seeds[4], (HOT, D), UNITS ** -0.5, 0.21875, ((0, 256),), (0, 1, 256, 6.0))
    hot_index = draw_hot_index(jax.random.fold_in(seeds[10], 71), 0)
    cold_gate = centred(seeds[6], (D, UNITS), D ** -0.5, 0.0625, ((0, 64), (1, 4)))
    cold_up = centred(seeds[7], (D, UNITS), D ** -0.5, 0.0625, ((0, 64), (1, 4)))
    cold_down = heavy_noise(seeds[8], (UNITS, D), UNITS ** -0.5, 0.125, ((0, 4), (1, 64)), (0, 1, 64, 4.0))
    block_mask = draw_block_mask(jax.random.fold_in(seeds[10], 71), 0)
    return {"tokens": tokens, "norm_gain": norm_gain, "hot_gate": hot_gate, "hot_up": hot_up, "hot_down": hot_down, "hot_index": hot_index, "cold_gate": cold_gate, "cold_up": cold_up, "cold_down": cold_down, "block_mask": block_mask}


def reference(tokens, norm_gain, hot_gate, hot_up, hot_down, hot_index, cold_gate, cold_up, cold_down, block_mask):
    values = tokens.astype(jnp.float32)
    scale = lax.rsqrt(lax.optimization_barrier(jnp.mean(values * values, axis=1, keepdims=True)) + 1e-05)
    normed = (values * scale * norm_gain.astype(jnp.float32)[None, :]).astype(jnp.bfloat16)
    dims = (((1,), (1,)), ((), ()))
    gate_hot = lax.dot_general(normed, hot_gate, dims, preferred_element_type=jnp.float32)
    up_hot = lax.dot_general(normed, hot_up, dims, preferred_element_type=jnp.float32)
    hidden_hot = (jax.nn.silu(gate_hot) * up_hot).astype(jnp.bfloat16)
    out_hot = jnp.dot(hidden_hot, hot_down, preferred_element_type=jnp.float32)
    is_hot = jnp.zeros((UNITS,), jnp.float32).at[hot_index.astype(jnp.int32)].set(1.0)
    live = jnp.repeat(block_mask, BLOCK, axis=1).astype(jnp.float32) * (1.0 - is_hot)[None, :]
    gate_cold = jnp.dot(normed, cold_gate, preferred_element_type=jnp.float32)
    up_cold = jnp.dot(normed, cold_up, preferred_element_type=jnp.float32)
    hidden_cold = (jax.nn.silu(gate_cold) * up_cold * live).astype(jnp.bfloat16)
    out_cold = jnp.dot(hidden_cold, cold_down, preferred_element_type=jnp.float32)
    return (out_hot + out_cold).astype(jnp.bfloat16)
```

```python
import functools

import jax
import jax.numpy as jnp
from jax import lax
from jax.experimental import pallas as pl
from jax.experimental.pallas import tpu as pltpu
from jax.sharding import PartitionSpec as P

MESH = pl.DeviceIdType.MESH
F32 = jnp.float32
BF16 = jnp.bfloat16
RING = 8
HALF = 7
CAP = 14
LANES = 128
EPS = 1e-05
CHUNK = 1024


def silu(v):
    return v / (1.0 + jnp.exp(-v))


def place(index):
    return pl.ds(pl.multiple_of(index * LANES, LANES), LANES)


def kernel(
    tok_hbm,
    gain_hbm,
    hg_hbm,
    hu_hbm,
    hd_hbm,
    hidx_hbm,
    cg_hbm,
    cu_hbm,
    cd_hbm,
    mask_hbm,
    out_ref,
    tok,
    gain,
    hw,
    hidx,
    cg,
    cu,
    cd,
    msk,
    mpad,
    s1,
    r1,
    s2,
    r2,
    h3,
    h4,
    hdp,
    hh,
    zs,
    zr,
    fs,
    fr,
    load_sem,
    own_sem,
    s1_send,
    s1_recv,
    s2_send,
    s2_recv,
    h3_send,
    h3_recv,
    h4_send,
    h4_recv,
    hd_send,
    hd_recv,
    hh_send,
    hh_recv,
    zs_send,
    zs_recv,
    fs_send,
    fs_recv,
):
    hot = lax.axis_index("hot")
    cold = lax.axis_index("cold")
    z = lax.div(hot, RING)
    p = lax.rem(hot, RING)
    seqs, features = tok.shape
    blocks_here = msk.shape[0]

    def ring(base, k):
        return lax.rem(base + k, RING)

    def remote(src, dst, send, recv, hot_to, cold_to):
        return pltpu.make_async_remote_copy(
            src_ref=src,
            dst_ref=dst,
            send_sem=send,
            recv_sem=recv,
            device_id=(hot_to, cold_to),
            device_id_type=MESH,
        )

    loads = [
        (mask_hbm, msk),
        (tok_hbm, tok),
        (gain_hbm, gain),
        (cg_hbm, cg),
        (cu_hbm, cu),
        (hg_hbm, hw.at[pl.ds(0, 16)]),
        (hu_hbm, hw.at[pl.ds(16, 16)]),
        (hidx_hbm, hidx),
        (cd_hbm, cd),
    ]
    load = [
        pltpu.make_async_copy(src, dst, load_sem.at[i])
        for i, (src, dst) in enumerate(loads)
    ]
    for copy in load:
        copy.start()

    def own_piece(zz):
        return pltpu.make_async_copy(
            hd_hbm.at[:, place(zz * RING + p)], hdp.at[p, zz], own_sem.at[zz]
        )

    for zz in range(RING):
        own_piece(zz).start()

    barrier = pltpu.get_barrier_semaphore()
    for k in range(1, RING):
        pl.semaphore_signal(
            barrier, inc=1, device_id=(z * RING + ring(p, k), cold), device_id_type=MESH
        )
        pl.semaphore_signal(
            barrier, inc=1, device_id=(ring(z, k) * RING + p, cold), device_id_type=MESH
        )
    for k in range(1, 4):
        pl.semaphore_signal(
            barrier, inc=1, device_id=(hot, lax.rem(cold + k, 4)), device_id_type=MESH
        )

    load[0].wait()
    mpad[...] = jnp.zeros_like(mpad)
    mpad[0:blocks_here, 0:seqs] = msk[...]
    block_id = lax.broadcasted_iota(jnp.int32, mpad.shape, 0)
    lane_id = lax.broadcasted_iota(jnp.int32, mpad.shape, 1)
    active = mpad[...]
    step = 1
    while step < LANES:
        active = jnp.maximum(active, pltpu.roll(active, step, 1))
        step *= 2
    upto = active
    step = 1
    while step < 32:
        upto = upto + jnp.where(block_id >= step, pltpu.roll(upto, step, 0), 0)
        step *= 2
    ahead = upto - active
    rank = jnp.where(active > 0, ahead, upto[31:32] + block_id - ahead)
    order = jnp.sum(jnp.where(rank == lane_id, block_id, 0), axis=0, keepdims=True)
    slots = [order[0, k] for k in range(CAP)]

    load[1].wait()
    load[2].wait()

    def add_squares(c, total):
        x = tok[:, place(c)].astype(F32)
        return total + x * x

    squares = lax.fori_loop(
        0, features // LANES, add_squares, jnp.zeros((seqs, LANES), F32), unroll=8
    )
    scale = lax.rsqrt(jnp.sum(squares, axis=1, keepdims=True) / features + EPS)
    mine = (tok[:, place(hot)].astype(F32) * scale * gain[:, place(hot)]).astype(BF16)

    load[3].wait()
    load[4].wait()
    for k in range(CAP):
        half, j = divmod(k, HALF)
        cols = pl.ds(slots[k] * LANES, LANES)
        both = jnp.concatenate([cg[:, cols], cu[:, cols]], axis=1)
        part = jnp.dot(mine, both, preferred_element_type=F32).astype(BF16)
        for r in range(4):
            s1[4 * half + r, j, 0] = part[16 * r : 16 * r + 16, :LANES]
            s1[4 * half + r, j, 1] = part[16 * r : 16 * r + 16, LANES:]

    pl.semaphore_wait(barrier, 17)

    def s1_copy(k):
        to = ring(p, k)
        return remote(
            s1.at[to], r1.at[p], s1_send.at[k], s1_recv.at[p], z * RING + to, cold
        )

    for k in range(1, RING):
        s1_copy(k).start()

    def hd_copy(k, zz):
        to = ring(p, k)
        return remote(
            hd_hbm.at[:, place(zz * RING + to)],
            hdp.at[p, zz],
            hd_send.at[k],
            hd_recv.at[p],
            z * RING + to,
            cold,
        )

    for k in range(1, RING):

        @pl.loop(0, RING)
        def _(zz):
            hd_copy(k, zz).start()

    load[5].wait()
    load[6].wait()

    def hot_chunk(c, total):
        cols = pl.ds(pl.multiple_of(c * CHUNK, CHUNK), CHUNK)
        normed = (tok[:, cols].astype(F32) * scale * gain[:, cols]).astype(BF16)
        return total + lax.dot_general(
            hw[:, cols], normed, (((1,), (1,)), ((), ())), preferred_element_type=F32
        )

    hot_t = lax.fori_loop(
        0, features // CHUNK, hot_chunk, jnp.zeros((32, seqs), F32)
    )
    hidden_t = silu(hot_t[:16]) * hot_t[16:]
    hh[p] = jnp.concatenate([hidden_t, jnp.zeros_like(hidden_t)], axis=1).astype(BF16)

    def hh_copy(k):
        to = ring(p, k)
        return remote(
            hh.at[p], hh.at[p], hh_send.at[k], hh_recv.at[p], z * RING + to, cold
        )

    for k in range(1, RING):
        hh_copy(k).start()

    busy = z != p
    j_own = lax.rem(z - p - 1 + 2 * RING, RING)
    half_own = lax.div(p, 4)
    row_own = lax.rem(p, 4)
    slot_own = half_own * HALF + j_own
    block_own = jnp.int32(0)
    for k in range(CAP):
        block_own = jnp.where(slot_own == k, slots[k], block_own)
    load[7].wait()
    unit = (cold * blocks_here + block_own) * LANES + lax.broadcasted_iota(
        jnp.int32, (LANES, LANES), 0
    )

    def match(c, found):
        return jnp.where(hidx[:, place(c)] == unit, 1.0, found)

    found = lax.fori_loop(
        0, hidx.shape[1] // LANES, match, jnp.zeros((LANES, LANES), F32), unroll=4
    )
    hot_units = lax.dot_general(
        jnp.ones((8, LANES), BF16),
        found.astype(BF16),
        (((1,), (1,)), ((), ())),
        preferred_element_type=F32,
    )[0:1]
    chosen = jnp.sum(
        jnp.where(block_id == block_own, mpad[...], 0).astype(F32), axis=0, keepdims=True
    )
    row = lax.broadcasted_iota(jnp.int32, (16, LANES), 0) + row_own * 16
    column = lax.broadcasted_iota(jnp.int32, (16, LANES), 1)
    seq_live = jnp.sum(jnp.where(row == column, chosen, 0.0), axis=1, keepdims=True)
    live = seq_live * (1.0 - jnp.minimum(hot_units, 1.0))

    total = s1[p].astype(F32)
    for k in range(1, RING):
        src = ring(p, k)
        remote(
            s1.at[src], r1.at[src], s1_send.at[k], s1_recv.at[src], z * RING + src, cold
        ).wait_recv()
        total = total + r1[src].astype(F32)
    s2[...] = total.astype(BF16)

    def s2_copy(j):
        to = ring(p, 1 + j)
        return to, remote(
            s2.at[j], r2.at[z], s2_send.at[j], s2_recv.at[z], to * RING + p, cold
        )

    for j in range(HALF):
        to, copy = s2_copy(j)

        @pl.when(to != z)
        def _():
            copy.start()

    for zz in range(RING):
        own_piece(zz).wait()
    for k in range(1, RING):
        src = ring(p, k)
        remote(
            hdp.at[src], hdp.at[src], hd_send.at[k], hd_recv.at[src], z * RING + src, cold
        ).wait_recv()
        remote(
            hh.at[src], hh.at[src], hh_send.at[k], hh_recv.at[src], z * RING + src, cold
        ).wait_recv()
    hidden = jnp.transpose(hh[...].reshape(LANES, LANES).astype(F32))[:seqs].astype(BF16)
    for zz in range(0, RING, 2):
        down = jnp.concatenate(
            [
                hdp[:, zz].reshape(LANES, LANES),
                hdp[:, zz + 1].reshape(LANES, LANES),
            ],
            axis=1,
        )
        part = jnp.dot(hidden, down, preferred_element_type=F32).astype(BF16)
        zs[zz] = part[:, :LANES]
        zs[zz + 1] = part[:, LANES:]

    def zs_copy(k):
        to = ring(z, k)
        return remote(
            zs.at[to], zr.at[z], zs_send.at[k], zs_recv.at[z], to * RING + p, cold
        )

    for k in range(1, RING):
        zs_copy(k).start()

    def h3_copy(k):
        to = ring(z, k)
        return remote(
            h3.at[j_own],
            h3.at[j_own],
            h3_send.at[k],
            h3_recv.at[j_own],
            to * RING + p,
            cold,
        )

    @pl.when(busy)
    def _():
        both = s2[j_own].astype(F32)
        for k in range(1, RING):
            src = ring(z, k)
            remote(
                r2.at[src], r2.at[src], s2_send.at[0], s2_recv.at[src], src * RING + p, cold
            ).wait_recv()
            both = both + r2[src].astype(F32)
        h3[j_own] = (silu(both[0]) * both[1] * live).astype(BF16)
        for k in range(1, RING):
            h3_copy(k).start()

    hot_out = zs[z].astype(F32)
    for k in range(1, RING):
        src = ring(z, k)
        remote(
            zr.at[src], zr.at[src], zs_send.at[k], zs_recv.at[src], src * RING + p, cold
        ).wait_recv()
        hot_out = hot_out + zr[src].astype(F32)

    for j in range(HALF):
        src = ring(p, 1 + j)

        @pl.when(src != z)
        def _():
            remote(
                h3.at[j], h3.at[j], h3_send.at[1 + j], h3_recv.at[j], src * RING + p, cold
            ).wait_recv()

    def h4_copy(k):
        to = ring(p, k)
        return remote(
            h3, h4.at[p], h4_send.at[k], h4_recv.at[p], z * RING + to, cold
        )

    for k in range(1, RING):
        h4_copy(k).start()
    h4[p] = h3[...]
    load[8].wait()
    for k in range(1, RING):
        src = ring(p, k)
        remote(
            h3, h4.at[src], h4_send.at[k], h4_recv.at[src], z * RING + src, cold
        ).wait_recv()

    acc = hot_out
    for k in range(0, CAP, 2):
        left, right = [
            h4[4 * (i // HALF) : 4 * (i // HALF) + 4, i % HALF].reshape(seqs, LANES)
            for i in (k, k + 1)
        ]
        down = jnp.concatenate(
            [cd[pl.ds(slots[i] * LANES, LANES), :] for i in (k, k + 1)], axis=0
        )
        acc = acc + jnp.dot(
            jnp.concatenate([left, right], axis=1), down, preferred_element_type=F32
        )

    flipped = jnp.transpose(jnp.concatenate([acc, jnp.zeros_like(acc)], axis=0))
    for c in range(4):
        fs[c] = jnp.concatenate(
            [
                flipped[32 * c : 32 * c + 16, :seqs],
                flipped[32 * c + 16 : 32 * c + 32, :seqs],
            ],
            axis=1,
        )

    def fs_copy(k):
        to = lax.rem(cold + k, 4)
        return remote(fs.at[to], fr.at[cold], fs_send.at[k], fs_recv.at[cold], hot, to)

    for k in range(1, 4):
        fs_copy(k).start()
    result = fs[cold]
    for k in range(1, 4):
        src = lax.rem(cold + k, 4)
        remote(
            fr.at[src], fr.at[src], fs_send.at[k], fs_recv.at[src], hot, src
        ).wait_recv()
        result = result + fr[src]
    out_ref[0:16, :] = result[:, :seqs].astype(BF16)
    out_ref[16:32, :] = result[:, seqs:].astype(BF16)

    for k in range(1, RING):
        s1_copy(k).wait_send()
        remote(
            hdp.at[p], hdp.at[p], hd_send.at[k], hd_recv.at[p], z * RING + ring(p, k), cold
        ).wait_send()
        hh_copy(k).wait_send()
        zs_copy(k).wait_send()
        h4_copy(k).wait_send()
    for j in range(HALF):
        to, copy = s2_copy(j)

        @pl.when(to != z)
        def _():
            copy.wait_send()

    @pl.when(busy)
    def _():
        for k in range(1, RING):
            h3_copy(k).wait_send()

    for k in range(1, 4):
        fs_copy(k).wait_send()


def on_device(
    tokens,
    norm_gain,
    hot_gate,
    hot_up,
    hot_down,
    hot_index,
    cold_gate,
    cold_up,
    cold_down,
    block_mask,
):
    seqs, features = tokens.shape
    dma = pltpu.SemaphoreType.DMA
    any_space = pl.BlockSpec(memory_space=pl.ANY)
    return pl.pallas_call(
        kernel,
        out_shape=jax.ShapeDtypeStruct((32, seqs), BF16),
        in_specs=[any_space] * 10,
        out_specs=pl.BlockSpec(memory_space=pltpu.VMEM),
        scratch_shapes=[
            pltpu.VMEM(tokens.shape, BF16),
            pltpu.VMEM((1, features), F32),
            pltpu.VMEM((32, features), BF16),
            pltpu.VMEM((1, hot_index.shape[0]), jnp.int32),
            pltpu.VMEM(cold_gate.shape, BF16),
            pltpu.VMEM(cold_up.shape, BF16),
            pltpu.VMEM(cold_down.shape, BF16),
            pltpu.VMEM(block_mask.shape[::-1], jnp.int32),
            pltpu.VMEM((32, LANES), jnp.int32),
            pltpu.VMEM((RING, HALF, 2, 16, LANES), BF16),
            pltpu.VMEM((RING, HALF, 2, 16, LANES), BF16),
            pltpu.VMEM((HALF, 2, 16, LANES), BF16),
            pltpu.VMEM((RING, 2, 16, LANES), BF16),
            pltpu.VMEM((HALF, 16, LANES), BF16),
            pltpu.VMEM((RING, HALF, 16, LANES), BF16),
            pltpu.VMEM((RING, RING, 16, LANES), BF16),
            pltpu.VMEM((RING, 16, LANES), BF16),
            pltpu.VMEM((RING, seqs, LANES), BF16),
            pltpu.VMEM((RING, seqs, LANES), BF16),
            pltpu.VMEM((4, 16, LANES), F32),
            pltpu.VMEM((4, 16, LANES), F32),
            dma((9,)),
            dma((RING,)),
        ]
        + [dma((RING,))] * 14
        + [dma((4,))] * 2,
        compiler_params=pltpu.CompilerParams(collective_id=0, has_side_effects=True),
    )(
        tokens,
        norm_gain.reshape(1, -1),
        hot_gate,
        hot_up,
        hot_down,
        hot_index.reshape(1, -1),
        cold_gate,
        cold_up,
        cold_down,
        block_mask.T,
    ).T


def solution(mesh):
    rows = P(("hot", "cold"), None)
    return jax.shard_map(
        on_device,
        mesh=mesh,
        in_specs=(
            P(),
            P(),
            rows,
            rows,
            rows,
            P(),
            P("hot", "cold"),
            P("hot", "cold"),
            P("cold", "hot"),
            P(None, "cold"),
        ),
        out_specs=P(None, ("hot", "cold")),
        check_vma=False,
    )
```

```python
import functools

import jax
import jax.numpy as jnp
from jax import lax
from jax.experimental import pallas as pl
from jax.experimental.pallas import tpu as pltpu
from jax.sharding import PartitionSpec as P

MESH = pl.DeviceIdType.MESH
F32 = jnp.float32
BF16 = jnp.bfloat16
RING = 8
PAIRS = 7
CAP = 14
LANES = 128
EPS = 1e-05
CHUNK = 1024


def silu(v):
    return v / (1.0 + jnp.exp(-v))


def place(index):
    return pl.ds(pl.multiple_of(index * LANES, LANES), LANES)


def kernel(
    tok_hbm,
    gain_hbm,
    hg_hbm,
    hu_hbm,
    hd_hbm,
    hidx_hbm,
    cg_hbm,
    cu_hbm,
    cd_hbm,
    mask_hbm,
    out_ref,
    tok,
    gain,
    hw,
    hidx,
    cg,
    cu,
    cd,
    msk,
    mpad,
    s1,
    r1,
    s2,
    r2,
    h3,
    cds,
    cdr,
    hdp,
    hh,
    acc,
    fs,
    fr,
    load_sem,
    own_sem,
    s1_send,
    s1_recv,
    s2_send,
    s2_recv,
    h3_send,
    h3_recv,
    cd_send,
    cd_recv,
    hd_send,
    hd_recv,
    hh_send,
    hh_recv,
    fs_send,
    fs_recv,
):
    hot = lax.axis_index("hot")
    cold = lax.axis_index("cold")
    z = lax.div(hot, RING)
    p = lax.rem(hot, RING)
    core = lax.rem(cold, 2)
    seqs, features = tok.shape
    blocks_here = msk.shape[0]

    def ring(base, k):
        return lax.rem(base + k, RING)

    def swap(place_or_pair):
        return place_or_pair + core * (1 - 2 * lax.rem(place_or_pair, 2))

    pair = swap(p)
    works = pair < PAIRS

    def remote(src, dst, send, recv, hot_to, cold_to):
        return pltpu.make_async_remote_copy(
            src_ref=src,
            dst_ref=dst,
            send_sem=send,
            recv_sem=recv,
            device_id=(hot_to, cold_to),
            device_id_type=MESH,
        )

    def in_plane(to):
        return z * RING + to

    def along_z(to):
        return to * RING + p

    loads = [
        (mask_hbm, msk),
        (tok_hbm, tok),
        (gain_hbm, gain),
        (cg_hbm, cg),
        (cu_hbm, cu),
        (hg_hbm, hw.at[pl.ds(0, 16)]),
        (hu_hbm, hw.at[pl.ds(16, 16)]),
        (hidx_hbm, hidx),
        (cd_hbm, cd),
    ]
    load = [
        pltpu.make_async_copy(src, dst, load_sem.at[i])
        for i, (src, dst) in enumerate(loads)
    ]
    for copy in load:
        copy.start()

    def columns_of(zz):
        return pl.ds(pl.multiple_of(zz * RING * LANES, RING * LANES), RING * LANES)

    own_piece = pltpu.make_async_copy(
        hd_hbm.at[:, columns_of(z)], hdp.at[z], own_sem.at[0]
    )
    own_piece.start()

    barrier = pltpu.get_barrier_semaphore()

    def greet(hot_to, cold_to):
        pl.semaphore_signal(
            barrier, inc=1, device_id=(hot_to, cold_to), device_id_type=MESH
        )

    for k in range(1, RING):
        greet(along_z(ring(z, k)), cold)
    for k in range(RING):
        for c in range(4):
            if k + c:
                greet(in_plane(ring(p, k)), lax.rem(cold + c, 4))

    load[0].wait()
    mpad[...] = jnp.zeros_like(mpad)
    mpad[0:blocks_here, 0:seqs] = msk[...]
    block_id = lax.broadcasted_iota(jnp.int32, mpad.shape, 0)
    lane_id = lax.broadcasted_iota(jnp.int32, mpad.shape, 1)
    active = mpad[...]
    step = 1
    while step < LANES:
        active = jnp.maximum(active, pltpu.roll(active, step, 1))
        step *= 2
    upto = active
    step = 1
    while step < 32:
        upto = upto + jnp.where(block_id >= step, pltpu.roll(upto, step, 0), 0)
        step *= 2
    ahead = upto - active
    rank = jnp.where(active > 0, ahead, upto[31:32] + block_id - ahead)
    order = jnp.sum(jnp.where(rank == lane_id, block_id, 0), axis=0, keepdims=True)
    slots = [order[0, k] for k in range(CAP)]

    load[1].wait()
    load[2].wait()

    def add_squares(c, total):
        x = tok[:, place(c)].astype(F32)
        return total + x * x

    squares = lax.fori_loop(
        0, features // LANES, add_squares, jnp.zeros((seqs, LANES), F32), unroll=8
    )
    scale = lax.rsqrt(jnp.sum(squares, axis=1, keepdims=True) / features + EPS)
    mine = (tok[:, place(hot)].astype(F32) * scale * gain[:, place(hot)]).astype(BF16)

    load[3].wait()
    load[4].wait()
    for k in range(CAP):
        cols = pl.ds(slots[k] * LANES, LANES)
        both = jnp.concatenate([cg[:, cols], cu[:, cols]], axis=1)
        part = jnp.dot(mine, both, preferred_element_type=F32).astype(BF16)
        s1[k // 2, k % 2, 0] = part[:, :LANES]
        s1[k // 2, k % 2, 1] = part[:, LANES:]

    pl.semaphore_wait(barrier, 38)

    def s1_copy(k):
        to = ring(p, k)
        at = jnp.minimum(swap(to), PAIRS - 1)
        return to, remote(
            s1.at[at], r1.at[p], s1_send.at[k], s1_recv.at[p], in_plane(to), cold
        )

    def hd_copy(k):
        to = ring(z, k)
        return remote(
            hd_hbm.at[:, columns_of(to)],
            hdp.at[z],
            hd_send.at[k],
            hd_recv.at[z],
            along_z(to),
            cold,
        )

    for k in range(1, RING):
        to, copy = s1_copy(k)

        @pl.when(swap(to) < PAIRS)
        def _():
            copy.start()

    for k in range(1, RING):
        hd_copy(k).start()

    load[5].wait()
    load[6].wait()

    def hot_chunk(c, total):
        cols = pl.ds(pl.multiple_of(c * CHUNK, CHUNK), CHUNK)
        normed = (tok[:, cols].astype(F32) * scale * gain[:, cols]).astype(BF16)
        return total + lax.dot_general(
            hw[:, cols], normed, (((1,), (1,)), ((), ())), preferred_element_type=F32
        )

    hot_t = lax.fori_loop(
        0, features // CHUNK, hot_chunk, jnp.zeros((32, seqs), F32)
    )
    hidden_t = silu(hot_t[:16]) * hot_t[16:]
    hh[z] = jnp.concatenate([hidden_t, jnp.zeros_like(hidden_t)], axis=1).astype(BF16)

    def hh_copy(k):
        return remote(
            hh.at[z], hh.at[z], hh_send.at[k], hh_recv.at[z], along_z(ring(z, k)), cold
        )

    for k in range(1, RING):
        hh_copy(k).start()

    half = lax.rem(z, 2)
    rows = lax.div(z, 2)
    slot_own = jnp.minimum(pair, PAIRS - 1) * 2 + half
    block_own = jnp.int32(0)
    for k in range(CAP):
        block_own = jnp.where(slot_own == k, slots[k], block_own)
    load[7].wait()
    unit = (cold * blocks_here + block_own) * LANES + lax.broadcasted_iota(
        jnp.int32, (LANES, LANES), 0
    )

    def match(c, found):
        return jnp.where(hidx[:, place(c)] == unit, 1.0, found)

    found = lax.fori_loop(
        0, hidx.shape[1] // LANES, match, jnp.zeros((LANES, LANES), F32), unroll=4
    )
    hot_units = lax.dot_general(
        jnp.ones((8, LANES), BF16),
        found.astype(BF16),
        (((1,), (1,)), ((), ())),
        preferred_element_type=F32,
    )[0:1]
    chosen = jnp.sum(
        jnp.where(block_id == block_own, mpad[...], 0).astype(F32), axis=0, keepdims=True
    )
    row = lax.broadcasted_iota(jnp.int32, (16, LANES), 0) + rows * 16
    column = lax.broadcasted_iota(jnp.int32, (16, LANES), 1)
    seq_live = jnp.sum(jnp.where(row == column, chosen, 0.0), axis=1, keepdims=True)
    live = seq_live * (1.0 - jnp.minimum(hot_units, 1.0))

    load[8].wait()
    for k in range(CAP):
        block = cd[pl.ds(slots[k] * LANES, LANES), :]
        cds[k // 2, :, LANES * (k % 2) : LANES * (k % 2) + LANES] = jnp.transpose(block)

    @pl.when(works)
    def _():
        total = s1[jnp.minimum(pair, PAIRS - 1)].astype(F32)
        for k in range(1, RING):
            src = ring(p, k)
            remote(
                s1.at[0], r1.at[src], s1_send.at[k], s1_recv.at[src], in_plane(src), cold
            ).wait_recv()
            total = total + r1[src].astype(F32)
        total = total.astype(BF16)
        for r in range(4):
            for e in range(2):
                for g in range(2):
                    s2[2 * r + e, g] = total[e, g, 16 * r : 16 * r + 16]

    def s2_copy(k):
        to = ring(z, k)
        return remote(
            s2.at[to], r2.at[z], s2_send.at[k], s2_recv.at[z], along_z(to), cold
        )

    @pl.when(works)
    def _():
        for k in range(1, RING):
            s2_copy(k).start()

    def cd_copy(k):
        to = ring(p, k)
        at = jnp.minimum(swap(to), PAIRS - 1)
        return to, remote(
            cds.at[at], cdr.at[p], cd_send.at[k], cd_recv.at[p], in_plane(to), cold
        )

    for k in range(1, RING):
        to, copy = cd_copy(k)

        @pl.when(swap(to) < PAIRS)
        def _():
            copy.start()

    cdr[p] = cds[jnp.minimum(pair, PAIRS - 1)]

    piece = half * 4 + rows

    def h3_copy(k):
        return remote(
            h3.at[piece],
            h3.at[piece],
            h3_send.at[k],
            h3_recv.at[z],
            along_z(ring(z, k)),
            cold,
        )

    @pl.when(works)
    def _():
        both = s2[z].astype(F32)
        for k in range(1, RING):
            src = ring(z, k)
            remote(
                s2.at[src], r2.at[src], s2_send.at[k], s2_recv.at[src], along_z(src), cold
            ).wait_recv()
            both = both + r2[src].astype(F32)
        h3[piece] = (silu(both[0]) * both[1] * live).astype(BF16)
        for k in range(1, RING):
            h3_copy(k).start()

    own_piece.wait()
    for k in range(1, RING):
        src = ring(z, k)
        remote(
            hdp.at[src], hdp.at[src], hd_send.at[k], hd_recv.at[src], along_z(src), cold
        ).wait_recv()
        remote(
            hh.at[src], hh.at[src], hh_send.at[k], hh_recv.at[src], along_z(src), cold
        ).wait_recv()
    hidden = hh[...].reshape(LANES, LANES)[:, :seqs]
    for q in range(RING):
        down = hdp[:, :, LANES * q : LANES * q + LANES].reshape(LANES, LANES)
        acc[q] = jnp.dot(jnp.transpose(down), hidden, preferred_element_type=F32)

    @pl.when(works)
    def _():
        for k in range(1, RING):
            src = ring(p, k)
            remote(
                cds.at[0], cdr.at[src], cd_send.at[k], cd_recv.at[src], in_plane(src), cold
            ).wait_recv()

    @pl.when(works)
    def _():
        for k in range(1, RING):
            src = ring(z, k)
            remote(
                h3.at[piece], h3.at[piece], h3_send.at[k], h3_recv.at[src], along_z(src), cold
            ).wait_recv()

    @pl.when(works)
    def _():
        pair_hidden = jnp.concatenate(
            [h3[0:4].reshape(seqs, LANES), h3[4:8].reshape(seqs, LANES)], axis=1
        )
        for q in range(RING):
            acc[q] = acc[q] + lax.dot_general(
                cdr[q],
                pair_hidden,
                (((1,), (1,)), ((), ())),
                preferred_element_type=F32,
            )

    for q in range(RING):
        for c in range(4):
            fs[q, c] = jnp.concatenate(
                [acc[q, 32 * c : 32 * c + 16, :], acc[q, 32 * c + 16 : 32 * c + 32, :]],
                axis=1,
            ).astype(BF16)

    def fs_copy(k, c):
        to, cold_to = ring(p, k), lax.rem(cold + c, 4)
        return remote(
            fs.at[to, cold_to],
            fr.at[k * 4 + c - 1],
            fs_send,
            fs_recv,
            in_plane(to),
            cold_to,
        )

    others = [(k, c) for k in range(RING) for c in range(4) if k + c]
    for k, c in others:
        fs_copy(k, c).start()

    result = fs[p, cold].astype(F32)
    all_others = pltpu.make_async_copy(fr, fr, fs_recv)
    all_others.wait()
    for i in range(len(others)):
        result = result + fr[i].astype(F32)
    out_ref[0:16, :] = result[:, :seqs].astype(BF16)
    out_ref[16:32, :] = result[:, seqs:].astype(BF16)

    pltpu.make_async_copy(fr, fr, fs_send).wait()
    for k in range(1, RING):
        hd_copy(k).wait_send()
        hh_copy(k).wait_send()
        for to, copy in (s1_copy(k), cd_copy(k)):

            @pl.when(swap(to) < PAIRS)
            def _():
                copy.wait_send()

    @pl.when(works)
    def _():
        for k in range(1, RING):
            s2_copy(k).wait_send()
            h3_copy(k).wait_send()


def on_device(
    tokens,
    norm_gain,
    hot_gate,
    hot_up,
    hot_down,
    hot_index,
    cold_gate,
    cold_up,
    cold_down,
    block_mask,
):
    seqs, features = tokens.shape
    dma = pltpu.SemaphoreType.DMA
    any_space = pl.BlockSpec(memory_space=pl.ANY)
    return pl.pallas_call(
        kernel,
        out_shape=jax.ShapeDtypeStruct((32, seqs), BF16),
        in_specs=[any_space] * 10,
        out_specs=pl.BlockSpec(memory_space=pltpu.VMEM),
        scratch_shapes=[
            pltpu.VMEM(tokens.shape, BF16),
            pltpu.VMEM((1, features), F32),
            pltpu.VMEM((32, features), BF16),
            pltpu.VMEM((1, hot_index.shape[0]), jnp.int32),
            pltpu.VMEM(cold_gate.shape, BF16),
            pltpu.VMEM(cold_up.shape, BF16),
            pltpu.VMEM(cold_down.shape, BF16),
            pltpu.VMEM(block_mask.shape[::-1], jnp.int32),
            pltpu.VMEM((32, LANES), jnp.int32),
            pltpu.VMEM((PAIRS, 2, 2, seqs, LANES), BF16),
            pltpu.VMEM((RING, 2, 2, seqs, LANES), BF16),
            pltpu.VMEM((RING, 2, 16, LANES), BF16),
            pltpu.VMEM((RING, 2, 16, LANES), BF16),
            pltpu.VMEM((RING, 16, LANES), BF16),
            pltpu.VMEM((PAIRS, LANES, 2 * LANES), BF16),
            pltpu.VMEM((RING, LANES, 2 * LANES), BF16),
            pltpu.VMEM((RING, 16, RING * LANES), BF16),
            pltpu.VMEM((RING, 16, LANES), BF16),
            pltpu.VMEM((RING, LANES, seqs), F32),
            pltpu.VMEM((RING, 4, 16, LANES), BF16),
            pltpu.VMEM((RING * 4 - 1, 16, LANES), BF16),
            dma((9,)),
            dma((1,)),
        ]
        + [dma((RING,))] * 12
        + [dma, dma],
        compiler_params=pltpu.CompilerParams(collective_id=0, has_side_effects=True),
    )(
        tokens,
        norm_gain.reshape(1, -1),
        hot_gate,
        hot_up,
        hot_down,
        hot_index.reshape(1, -1),
        cold_gate,
        cold_up,
        cold_down,
        block_mask.T,
    ).T


def solution(mesh):
    rows = P(("hot", "cold"), None)
    return jax.shard_map(
        on_device,
        mesh=mesh,
        in_specs=(
            P(),
            P(),
            rows,
            rows,
            rows,
            P(),
            P("hot", "cold"),
            P("hot", "cold"),
            P("cold", "hot"),
            P(None, "cold"),
        ),
        out_specs=P(None, ("hot", "cold")),
        check_vma=False,
    )
```

```python
import functools

import jax
import jax.numpy as jnp
from jax import lax
from jax.experimental import pallas as pl
from jax.experimental.pallas import tpu as pltpu
from jax.sharding import PartitionSpec as P

MESH = pl.DeviceIdType.MESH
F32 = jnp.float32
BF16 = jnp.bfloat16
RING = 8
FAR_Z = (4, 3, 5, 2, 6, 1, 7)
FAR_PLANE = (5, 4, 3, 7, 2, 6, 1)
PAIRS = 7
CAP = 14
LANES = 128
EPS = 1e-05
CHUNK = 1024


def silu(v):
    return v / (1.0 + jnp.exp(-v))


def place(index):
    return pl.ds(pl.multiple_of(index * LANES, LANES), LANES)


def kernel(
    tok_hbm,
    gain_hbm,
    hg_hbm,
    hu_hbm,
    hd_hbm,
    hidx_hbm,
    cg_hbm,
    cu_hbm,
    cd_hbm,
    mask_hbm,
    out_ref,
    tok,
    gain,
    hw,
    hidx,
    cg,
    cu,
    cd,
    msk,
    mpad,
    s1,
    r1,
    s2,
    r2,
    h3,
    cds,
    cdr,
    hdp,
    hh,
    lv,
    acc,
    fs,
    fr,
    load_sem,
    own_sem,
    s1_send,
    s1_recv,
    s2_send,
    s2_recv,
    h3_send,
    h3_recv,
    cd_send,
    cd_recv,
    hd_send,
    hd_recv,
    hh_send,
    hh_recv,
    lv_send,
    lv_recv,
    fs_send,
    fs_recv,
):
    hot = lax.axis_index("hot")
    cold = lax.axis_index("cold")
    z = lax.div(hot, RING)
    p = lax.rem(hot, RING)
    x_hi = lax.div(cold, 2)
    core = lax.rem(cold, 2)
    adds = core == 1
    partner = x_hi * 2 + 1
    seqs, features = tok.shape
    blocks_here = msk.shape[0]

    def ring(base, k):
        return lax.rem(base + k, RING)

    def in_plane_at(k):
        dy, dx = divmod(k, 2)
        y, x = lax.div(p, 2), lax.rem(p, 2)
        return tuple(
            lax.rem(y + d, 4) * 2 + x + dx * (1 - 2 * x) for d in (dy, 4 - dy)
        )

    def swap(group, place_or_pair):
        return place_or_pair + group * (1 - 2 * lax.rem(place_or_pair, 2))

    def works(group):
        return swap(group, p) < PAIRS

    def pair_of(group, to):
        return jnp.minimum(swap(group, to), PAIRS - 1)

    def remote(src, dst, send, recv, hot_to, cold_to):
        return pltpu.make_async_remote_copy(
            src_ref=src,
            dst_ref=dst,
            send_sem=send,
            recv_sem=recv,
            device_id=(hot_to, cold_to),
            device_id_type=MESH,
        )

    def in_plane(to):
        return z * RING + to

    def along_z(to):
        return to * RING + p

    loads = [
        (mask_hbm, msk),
        (tok_hbm, tok),
        (gain_hbm, gain),
        (cg_hbm, cg),
        (cu_hbm, cu),
        (hg_hbm, hw.at[pl.ds(0, 16)]),
        (hu_hbm, hw.at[pl.ds(16, 16)]),
        (hidx_hbm, hidx),
        (cd_hbm, cd),
    ]
    load = [
        pltpu.make_async_copy(src, dst, load_sem.at[i])
        for i, (src, dst) in enumerate(loads)
    ]
    for copy in load:
        copy.start()

    def columns_of(zz):
        return pl.ds(pl.multiple_of(zz * RING * LANES, RING * LANES), RING * LANES)

    own_piece = pltpu.make_async_copy(
        hd_hbm.at[:, columns_of(z)], hdp.at[1, z], own_sem.at[0]
    )

    @pl.when(adds)
    def _():
        own_piece.start()

    barrier = pltpu.get_barrier_semaphore()

    def greet(hot_to, cold_to):
        pl.semaphore_signal(
            barrier, inc=1, device_id=(hot_to, cold_to), device_id_type=MESH
        )

    for k in FAR_Z:
        greet(along_z(ring(z, k)), partner)
    for k in FAR_PLANE:
        greet(in_plane(in_plane_at(k)[0]), partner)
        greet(in_plane(in_plane_at(k)[0]), (1 - x_hi) * 2 + 1)
    greet(hot, (1 - x_hi) * 2 + 1)

    @pl.when(adds)
    def _():
        for k in FAR_Z:
            greet(along_z(ring(z, k)), x_hi * 2)
        for k in (*FAR_PLANE, 0):
            greet(in_plane(in_plane_at(k)[0]), x_hi * 2)
            greet(in_plane(in_plane_at(k)[0]), (1 - x_hi) * 2)

    @pl.when(core == 0)
    def _():
        greet(hot, partner)

    load[0].wait()
    mpad[...] = jnp.zeros_like(mpad)
    mpad[0:blocks_here, 0:seqs] = msk[...]
    block_id = lax.broadcasted_iota(jnp.int32, mpad.shape, 0)
    lane_id = lax.broadcasted_iota(jnp.int32, mpad.shape, 1)
    active = mpad[...]
    step = 1
    while step < LANES:
        active = jnp.maximum(active, pltpu.roll(active, step, 1))
        step *= 2
    upto = active
    step = 1
    while step < 32:
        upto = upto + jnp.where(block_id >= step, pltpu.roll(upto, step, 0), 0)
        step *= 2
    ahead = upto - active
    rank = jnp.where(active > 0, ahead, upto[31:32] + block_id - ahead)
    order = jnp.sum(jnp.where(rank == lane_id, block_id, 0), axis=0, keepdims=True)
    slots = [order[0, k] for k in range(CAP)]

    load[1].wait()
    load[2].wait()

    def add_squares(c, total):
        x = tok[:, place(c)].astype(F32)
        return total + x * x

    squares = lax.fori_loop(
        0, features // LANES, add_squares, jnp.zeros((seqs, LANES), F32), unroll=8
    )
    scale = lax.rsqrt(jnp.sum(squares, axis=1, keepdims=True) / features + EPS)
    mine = (tok[:, place(hot)].astype(F32) * scale * gain[:, place(hot)]).astype(BF16)

    load[3].wait()
    load[4].wait()
    for k in range(CAP):
        cols = pl.ds(slots[k] * LANES, LANES)
        both = jnp.concatenate([cg[:, cols], cu[:, cols]], axis=1)
        part = jnp.dot(mine, both, preferred_element_type=F32).astype(BF16)
        s1[k // 2, k % 2, 0] = part[:, :LANES]
        s1[k // 2, k % 2, 1] = part[:, LANES:]

    @pl.when(adds)
    def _():
        pl.semaphore_wait(barrier, 45)

    @pl.when(core == 0)
    def _():
        pl.semaphore_wait(barrier, 23)

    def plane_copies(op):
        for k in (*FAR_PLANE, 0):
            to = in_plane_at(k)[0]
            sends = swap(core, to) < PAIRS
            if k == 0:
                sends = jnp.logical_and(sends, core == 0)
            op(k, to, sends)

    def s1_copy(k, to):
        return remote(
            s1.at[pair_of(core, to)],
            r1.at[core, p],
            s1_send.at[k],
            s1_recv.at[core, p],
            in_plane(to),
            partner,
        )

    def start_s1(k, to, sends):
        @pl.when(sends)
        def _():
            s1_copy(k, to).start()

    plane_copies(start_s1)

    def z_copies(op):
        for k in FAR_Z:
            op(k)

        @pl.when(core == 0)
        def _():
            op(0)

    def hd_copy(k):
        to = ring(z, k)
        return remote(
            hd_hbm.at[:, columns_of(to)],
            hdp.at[core, z],
            hd_send.at[k],
            hd_recv.at[core, z],
            along_z(to),
            partner,
        )

    z_copies(lambda k: hd_copy(k).start())

    load[5].wait()
    load[6].wait()

    def hot_chunk(c, total):
        cols = pl.ds(pl.multiple_of(c * CHUNK, CHUNK), CHUNK)
        normed = (tok[:, cols].astype(F32) * scale * gain[:, cols]).astype(BF16)
        return total + lax.dot_general(
            hw[:, cols], normed, (((1,), (1,)), ((), ())), preferred_element_type=F32
        )

    hot_t = lax.fori_loop(
        0, features // CHUNK, hot_chunk, jnp.zeros((32, seqs), F32)
    )
    hidden_t = silu(hot_t[:16]) * hot_t[16:]
    hh[core, z] = jnp.concatenate([hidden_t, jnp.zeros_like(hidden_t)], axis=1).astype(
        BF16
    )

    def hh_copy(k):
        return remote(
            hh.at[core, z],
            hh.at[core, z],
            hh_send.at[k],
            hh_recv.at[core, z],
            along_z(ring(z, k)),
            partner,
        )

    z_copies(lambda k: hh_copy(k).start())

    half = lax.rem(z, 2)
    rows = lax.div(z, 2)
    slot_own = pair_of(core, p) * 2 + half
    block_own = jnp.int32(0)
    for k in range(CAP):
        block_own = jnp.where(slot_own == k, slots[k], block_own)
    load[7].wait()
    unit = (cold * blocks_here + block_own) * LANES + lax.broadcasted_iota(
        jnp.int32, (LANES, LANES), 0
    )

    def match(c, found):
        return jnp.where(hidx[:, place(c)] == unit, 1.0, found)

    found = lax.fori_loop(
        0, hidx.shape[1] // LANES, match, jnp.zeros((LANES, LANES), F32), unroll=4
    )
    hot_units = lax.dot_general(
        jnp.ones((8, LANES), BF16),
        found.astype(BF16),
        (((1,), (1,)), ((), ())),
        preferred_element_type=F32,
    )[0:1]
    chosen = jnp.sum(
        jnp.where(block_id == block_own, mpad[...], 0).astype(F32), axis=0, keepdims=True
    )
    row = lax.broadcasted_iota(jnp.int32, (16, LANES), 0) + rows * 16
    column = lax.broadcasted_iota(jnp.int32, (16, LANES), 1)
    seq_live = jnp.sum(jnp.where(row == column, chosen, 0.0), axis=1, keepdims=True)
    lv[core] = (seq_live * (1.0 - jnp.minimum(hot_units, 1.0))).astype(BF16)
    lv_copy = remote(lv.at[0], lv.at[0], lv_send, lv_recv, hot, partner)

    @pl.when(core == 0)
    def _():
        lv_copy.start()

    load[8].wait()
    for k in range(CAP):
        block = cd[pl.ds(slots[k] * LANES, LANES), :]
        cds[k // 2, :, LANES * (k % 2) : LANES * (k % 2) + LANES] = jnp.transpose(block)

    def cd_copy(k, to):
        return remote(
            cds.at[pair_of(core, to)],
            cdr.at[core, p],
            cd_send.at[k],
            cd_recv.at[core, p],
            in_plane(to),
            partner,
        )

    def start_cd(k, to, sends):
        @pl.when(sends)
        def _():
            cd_copy(k, to).start()

    def s2_copy(group, k):
        to = ring(z, k)
        return remote(
            s2.at[group, to],
            r2.at[group, z],
            s2_send.at[group, k],
            s2_recv.at[group, z],
            along_z(to),
            partner,
        )

    piece = half * 4 + rows

    def h3_copy(group, k):
        return remote(
            h3.at[group, piece],
            h3.at[group, piece],
            h3_send.at[group, k],
            h3_recv.at[group, z],
            along_z(ring(z, k)),
            partner,
        )

    def fs_copy(k, other, core_to):
        cold_to = lax.rem(x_hi + other, 2) * 2 + core_to
        return remote(
            fs.at[4 * k + cold_to],
            fr.at[2 * k + other],
            fs_send,
            fs_recv,
            in_plane(in_plane_at(k)[0]),
            cold_to,
        )

    @pl.when(core == 0)
    def _():
        plane_copies(start_cd)

    @pl.when(adds)
    def _():
        for group in (1, 0):

            @pl.when(works(group))
            def _():
                if group:
                    total = s1[pair_of(1, p)].astype(F32)
                else:
                    total = jnp.zeros(s1.shape[1:], F32)
                for k in range(group, RING):
                    src = in_plane_at(k)[1]
                    remote(
                        s1.at[0],
                        r1.at[group, src],
                        s1_send.at[k],
                        s1_recv.at[group, src],
                        hot,
                        partner,
                    ).wait_recv()
                    total = total + r1[group, src].astype(F32)
                total = total.astype(BF16)
                for r in range(4):
                    for e in range(2):
                        for g in range(2):
                            s2[group, 2 * r + e, g] = total[e, g, 16 * r : 16 * r + 16]
                for k in FAR_Z:
                    s2_copy(group, k).start()

        plane_copies(start_cd)
        cdr[1, p] = cds[pair_of(1, p)]

        remote(lv.at[0], lv.at[0], lv_send, lv_recv, hot, partner).wait_recv()
        for group in (1, 0):

            @pl.when(works(group))
            def _():
                both = s2[group, z].astype(F32)
                for k in range(1, RING):
                    src = ring(z, k)
                    remote(
                        s2.at[group, src],
                        r2.at[group, src],
                        s2_send.at[group, k],
                        s2_recv.at[group, src],
                        hot,
                        partner,
                    ).wait_recv()
                    both = both + r2[group, src].astype(F32)
                live = lv[group].astype(F32)
                h3[group, piece] = (silu(both[0]) * both[1] * live).astype(BF16)
                for k in FAR_Z:
                    h3_copy(group, k).start()

        own_piece.wait()
        for group in range(2):
            for k in range(group, RING):
                src = ring(z, k)
                remote(
                    hdp.at[group, src],
                    hdp.at[group, src],
                    hd_send.at[k],
                    hd_recv.at[group, src],
                    hot,
                    partner,
                ).wait_recv()
                remote(
                    hh.at[group, src],
                    hh.at[group, src],
                    hh_send.at[k],
                    hh_recv.at[group, src],
                    hot,
                    partner,
                ).wait_recv()
        hidden = hh[...].reshape(2 * LANES, LANES)[:, :seqs]
        for q in range(RING):
            down = hdp[:, :, :, LANES * q : LANES * q + LANES].reshape(2 * LANES, LANES)
            acc[q] = jnp.dot(jnp.transpose(down), hidden, preferred_element_type=F32)

        def await_pair(group):
            @pl.when(works(group))
            def _():
                for k in range(group, RING):
                    src = in_plane_at(k)[1]
                    remote(
                        cds.at[0],
                        cdr.at[group, src],
                        cd_send.at[k],
                        cd_recv.at[group, src],
                        hot,
                        partner,
                    ).wait_recv()
                for k in range(1, RING):
                    src = ring(z, k)
                    remote(
                        h3.at[group, piece],
                        h3.at[group, piece],
                        h3_send.at[group, k],
                        h3_recv.at[group, src],
                        hot,
                        partner,
                    ).wait_recv()

        def pair_hidden(group):
            return jnp.concatenate(
                [
                    h3[group, 0:4].reshape(seqs, LANES),
                    h3[group, 4:8].reshape(seqs, LANES),
                ],
                axis=1,
            )

        def pair_term(group, values, to):
            term = lax.dot_general(
                cdr[group, to],
                values,
                (((1,), (1,)), ((), ())),
                preferred_element_type=F32,
            )
            return acc[to] + jnp.where(works(group), term, 0.0)

        await_pair(1)
        values = pair_hidden(1)
        for q in range(RING):
            acc[q] = pair_term(1, values, q)
        await_pair(0)

        values = pair_hidden(0)
        terms = [pair_term(0, values, in_plane_at(k)[0]) for k in (*FAR_PLANE, 0)]
        for k, term in zip((*FAR_PLANE, 0), terms):
            for c in range(4):
                fs[4 * k + c] = jnp.concatenate(
                    [term[32 * c : 32 * c + 16], term[32 * c + 16 : 32 * c + 32]], axis=1
                ).astype(BF16)
            for other, core_to in ((1, 0), (1, 1), (0, 0), (0, 1)):
                if k + other or not core_to:
                    fs_copy(k, other, core_to).start()

        fr[0] = fs[cold]

    @pl.when(adds)
    def _():
        landed = fr.at[pl.ds(1, 2 * RING - 1)]
        pltpu.make_async_copy(landed, landed, fs_recv).wait()

    @pl.when(core == 0)
    def _():
        pltpu.make_async_copy(fr, fr, fs_recv).wait()

    result = fr[0].astype(F32)
    for i in range(1, 2 * RING):
        result = result + fr[i].astype(F32)
    out_ref[0:16, :] = result[:, :seqs].astype(BF16)
    out_ref[16:32, :] = result[:, seqs:].astype(BF16)

    def drain(k, to, sends):
        @pl.when(sends)
        def _():
            s1_copy(k, to).wait_send()
            cd_copy(k, to).wait_send()

    plane_copies(drain)
    z_copies(lambda k: hd_copy(k).wait_send())
    z_copies(lambda k: hh_copy(k).wait_send())

    @pl.when(core == 0)
    def _():
        lv_copy.wait_send()

    @pl.when(adds)
    def _():
        for group in range(2):

            @pl.when(works(group))
            def _():
                for k in FAR_Z:
                    s2_copy(group, k).wait_send()
                    h3_copy(group, k).wait_send()

        sent = fs.at[pl.ds(0, 4 * RING - 1)]
        pltpu.make_async_copy(sent, sent, fs_send).wait()


def on_device(
    tokens,
    norm_gain,
    hot_gate,
    hot_up,
    hot_down,
    hot_index,
    cold_gate,
    cold_up,
    cold_down,
    block_mask,
):
    seqs, features = tokens.shape
    dma = pltpu.SemaphoreType.DMA
    any_space = pl.BlockSpec(memory_space=pl.ANY)
    return pl.pallas_call(
        kernel,
        out_shape=jax.ShapeDtypeStruct((32, seqs), BF16),
        in_specs=[any_space] * 10,
        out_specs=pl.BlockSpec(memory_space=pltpu.VMEM),
        scratch_shapes=[
            pltpu.VMEM(tokens.shape, BF16),
            pltpu.VMEM((1, features), F32),
            pltpu.VMEM((32, features), BF16),
            pltpu.VMEM((1, hot_index.shape[0]), jnp.int32),
            pltpu.VMEM(cold_gate.shape, BF16),
            pltpu.VMEM(cold_up.shape, BF16),
            pltpu.VMEM(cold_down.shape, BF16),
            pltpu.VMEM(block_mask.shape[::-1], jnp.int32),
            pltpu.VMEM((32, LANES), jnp.int32),
            pltpu.VMEM((PAIRS, 2, 2, seqs, LANES), BF16),
            pltpu.VMEM((2, RING, 2, 2, seqs, LANES), BF16),
            pltpu.VMEM((2, RING, 2, 16, LANES), BF16),
            pltpu.VMEM((2, RING, 2, 16, LANES), BF16),
            pltpu.VMEM((2, RING, 16, LANES), BF16),
            pltpu.VMEM((PAIRS, LANES, 2 * LANES), BF16),
            pltpu.VMEM((2, RING, LANES, 2 * LANES), BF16),
            pltpu.VMEM((2, RING, 16, RING * LANES), BF16),
            pltpu.VMEM((2, RING, 16, LANES), BF16),
            pltpu.VMEM((2, 16, LANES), BF16),
            pltpu.VMEM((RING, LANES, seqs), F32),
            pltpu.VMEM((RING * 4, 16, LANES), BF16),
            pltpu.VMEM((2 * RING, 16, LANES), BF16),
            dma((9,)),
            dma((1,)),
            dma((RING,)),
            dma((2, RING)),
            dma((2, RING)),
            dma((2, RING)),
            dma((2, RING)),
            dma((2, RING)),
            dma((RING,)),
            dma((2, RING)),
            dma((RING,)),
            dma((2, RING)),
            dma((RING,)),
            dma((2, RING)),
            dma,
            dma,
            dma,
            dma,
        ],
        compiler_params=pltpu.CompilerParams(
            collective_id=0, has_side_effects=True, vmem_limit_bytes=55218 * 1024
        ),
    )(
        tokens,
        norm_gain.reshape(1, -1),
        hot_gate,
        hot_up,
        hot_down,
        hot_index.reshape(1, -1),
        cold_gate,
        cold_up,
        cold_down,
        block_mask.T,
    ).T


def solution(mesh):
    rows = P(("hot", "cold"), None)
    return jax.shard_map(
        on_device,
        mesh=mesh,
        in_specs=(
            P(),
            P(),
            rows,
            rows,
            rows,
            P(),
            P("hot", "cold"),
            P("hot", "cold"),
            P("cold", "hot"),
            P(None, "cold"),
        ),
        out_specs=P(None, ("hot", "cold")),
        check_vma=False,
    )
```

```python
import functools

import jax
import jax.numpy as jnp
from jax import lax
from jax.experimental import pallas as pl
from jax.experimental.pallas import tpu as pltpu
from jax.sharding import PartitionSpec as P

MESH = pl.DeviceIdType.MESH
F32 = jnp.float32
BF16 = jnp.bfloat16
RING = 8
FAR_Z = (4, 3, 5, 2, 6, 1, 7)
FAR_PLANE = (5, 4, 3, 7, 2, 6, 1)
NEAR_PLANE = (1, 2, 6, 3, 7, 4, 5)
EARLY_Z = (4, 2, 6)
LATE_Z = (3, 5, 1, 7)
Z_FIRST = 2
PAIRS = 7
CAP = 14
LANES = 128
EPS = 1e-05
CHUNK = 1024


def silu(v):
    return v / (1.0 + jnp.exp(-v))


def place(index):
    return pl.ds(pl.multiple_of(index * LANES, LANES), LANES)


def kernel(
    tok_hbm,
    gain_hbm,
    hg_hbm,
    hu_hbm,
    hd_hbm,
    hidx_hbm,
    cg_hbm,
    cu_hbm,
    cd_hbm,
    mask_hbm,
    out_ref,
    tok,
    gain,
    hw,
    hidx,
    cgu,
    cd,
    msk,
    mpad,
    s1,
    r1,
    rb,
    sq,
    s2,
    r2,
    h3,
    cds,
    cdr,
    hdp,
    hh,
    lv,
    acc,
    fs,
    fr,
    load_sem,
    s1_send,
    s1_recv,
    sb_send,
    sb_recv,
    sq_send,
    s2_send,
    r2_recv,
    h3_send,
    h3_recv,
    cd_send,
    cd_recv,
    hd_send,
    hd_recv,
    hh_send,
    hh_recv,
    lv_send,
    lv_recv,
    go,
    fs_send,
    fs_recv,
):
    hot = lax.axis_index("hot")
    cold = lax.axis_index("cold")
    z = lax.div(hot, RING)
    p = lax.rem(hot, RING)
    x_hi = lax.div(cold, 2)
    core = lax.rem(cold, 2)
    adds = core == 1
    partner = x_hi * 2 + 1
    seqs, features = tok.shape
    blocks_here = msk.shape[0]

    def ring(base, k):
        return lax.rem(base + k, RING)

    def in_plane_at(k):
        dy, dx = divmod(k, 2)
        y, x = lax.div(p, 2), lax.rem(p, 2)
        return tuple(
            lax.rem(y + d, 4) * 2 + x + dx * (1 - 2 * x) for d in (dy, 4 - dy)
        )

    def swap(group, place_or_pair):
        return 7 - place_or_pair + group * (2 * place_or_pair - 7)

    def works(group):
        return swap(group, p) < PAIRS

    def pair_of(group, to):
        return jnp.minimum(swap(group, to), PAIRS - 1)

    def remote(src, dst, send, recv, hot_to, cold_to):
        return pltpu.make_async_remote_copy(
            src_ref=src,
            dst_ref=dst,
            send_sem=send,
            recv_sem=recv,
            device_id=(hot_to, cold_to),
            device_id_type=MESH,
        )

    def landed(ref, sem):
        pltpu.make_async_copy(ref, ref, sem).wait()

    def in_plane(to):
        return z * RING + to

    def along_z(to):
        return to * RING + p

    loads = [
        (mask_hbm, msk, 0),
        (tok_hbm, tok, 1),
        (gain_hbm, gain, 2),
        (cg_hbm, cgu.at[0], 3),
        (cu_hbm, cgu.at[1], 3),
        (hg_hbm, hw.at[pl.ds(0, 16)], 4),
        (hu_hbm, hw.at[pl.ds(16, 16)], 4),
        (hidx_hbm, hidx, 5),
        (cd_hbm, cd, 6),
    ]
    for src, dst, sem in loads:
        pltpu.make_async_copy(src, dst, load_sem.at[sem]).start()

    def columns_of(zz):
        return pl.ds(pl.multiple_of(zz * RING * LANES, RING * LANES), RING * LANES)

    own_piece = pltpu.make_async_copy(
        hd_hbm.at[:, columns_of(z)], hdp.at[RING + z], load_sem.at[7]
    )

    @pl.when(adds)
    def _():
        own_piece.start()

    barrier = pltpu.get_barrier_semaphore()

    def greet(hot_to, cold_to):
        pl.semaphore_signal(
            barrier, inc=1, device_id=(hot_to, cold_to), device_id_type=MESH
        )

    for k in FAR_Z:
        greet(along_z(ring(z, k)), partner)
    for k in FAR_PLANE:
        greet(in_plane(in_plane_at(k)[0]), partner)
        greet(in_plane(in_plane_at(k)[0]), (1 - x_hi) * 2 + 1)
    greet(hot, (1 - x_hi) * 2 + 1)

    @pl.when(adds)
    def _():
        for k in FAR_Z:
            greet(along_z(ring(z, k)), x_hi * 2)
        for k in (*FAR_PLANE, 0):
            greet(in_plane(in_plane_at(k)[0]), x_hi * 2)
            greet(in_plane(in_plane_at(k)[0]), (1 - x_hi) * 2)

    @pl.when(core == 0)
    def _():
        greet(hot, partner)

    landed(msk, load_sem.at[0])
    mpad[...] = jnp.zeros_like(mpad)
    mpad[0:blocks_here, 0:seqs] = msk[...]
    block_id = lax.broadcasted_iota(jnp.int32, mpad.shape, 0)
    lane_id = lax.broadcasted_iota(jnp.int32, mpad.shape, 1)
    active = mpad[...]
    step = 1
    while step < LANES:
        active = jnp.maximum(active, pltpu.roll(active, step, 1))
        step *= 2
    upto = active
    step = 1
    while step < 32:
        upto = upto + jnp.where(block_id >= step, pltpu.roll(upto, step, 0), 0)
        step *= 2
    ahead = upto - active
    rank = jnp.where(active > 0, ahead, upto[31:32] + block_id - ahead)
    order = jnp.sum(jnp.where(rank == lane_id, block_id, 0), axis=0, keepdims=True)
    slots = [order[0, k] for k in range(CAP)]

    landed(tok, load_sem.at[1])
    landed(gain, load_sem.at[2])

    def add_squares(c, total):
        x = tok[:, place(c)].astype(F32)
        return total + x * x

    squares = lax.fori_loop(
        0, features // LANES, add_squares, jnp.zeros((seqs, LANES), F32), unroll=8
    )
    scale = lax.rsqrt(jnp.sum(squares, axis=1, keepdims=True) / features + EPS)
    mine = (tok[:, place(hot)].astype(F32) * scale * gain[:, place(hot)]).astype(BF16)

    landed(cgu, load_sem.at[3])
    for k in range(CAP):
        cols = pl.ds(slots[k] * LANES, LANES)
        both = jnp.concatenate([cgu[0, :, cols], cgu[1, :, cols]], axis=1)
        part = jnp.dot(mine, both, preferred_element_type=F32).astype(BF16)
        pair, half = divmod(k, 2)
        for r in range(4):
            at = (2 * r + half - pair) % RING
            s1[pair, at, 0] = part[16 * r : 16 * r + 16, :LANES]
            s1[pair, at, 1] = part[16 * r : 16 * r + 16, LANES:]

    @pl.when(adds)
    def _():
        pl.semaphore_wait(barrier, 45)

    @pl.when(core == 0)
    def _():
        pl.semaphore_wait(barrier, 23)

    def plane_copies(order, op):
        for k in (*order, 0):
            to = in_plane_at(k)[0]
            sends = swap(core, to) < PAIRS
            if k == 0:
                sends = jnp.logical_and(sends, core == 0)
            op(k, to, sends)

    def s1_copy(k, to):
        return remote(
            s1.at[pair_of(core, to), pl.ds(Z_FIRST, RING - Z_FIRST)],
            r1.at[core, p],
            s1_send,
            s1_recv.at[core],
            in_plane(to),
            partner,
        )

    def start_s1(k, to, sends):
        @pl.when(sends)
        def _():
            s1_copy(k, to).start()

    plane_copies(NEAR_PLANE, start_s1)

    def z_copies(order, op):
        for k in order:
            op(k)

        @pl.when(core == 0)
        def _():
            op(0)

    def pair_at(zz, b):
        return lax.rem(zz + RING - b, RING)

    def sb_copies(op):
        def each(k):
            to = ring(z, k)
            for b in range(Z_FIRST):
                pair = pair_at(to, b)
                copy = remote(
                    s1.at[jnp.minimum(pair, PAIRS - 1), b],
                    rb.at[core, b, z],
                    sb_send,
                    sb_recv.at[core, b],
                    along_z(to),
                    partner,
                )

                @pl.when(pair < PAIRS)
                def _():
                    op(copy)

        z_copies(FAR_Z, each)

    sb_copies(lambda copy: copy.start())

    def hd_copy(k):
        to = ring(z, k)
        return remote(
            hd_hbm.at[:, columns_of(to)],
            hdp.at[core * RING + z],
            hd_send,
            hd_recv,
            along_z(to),
            partner,
        )

    z_copies(EARLY_Z, lambda k: hd_copy(k).start())

    landed(hw, load_sem.at[4])

    def hot_chunk(c, total):
        cols = pl.ds(pl.multiple_of(c * CHUNK, CHUNK), CHUNK)
        normed = (tok[:, cols].astype(F32) * scale * gain[:, cols]).astype(BF16)
        return total + lax.dot_general(
            hw[:, cols], normed, (((1,), (1,)), ((), ())), preferred_element_type=F32
        )

    hot_t = lax.fori_loop(
        0, features // CHUNK, hot_chunk, jnp.zeros((32, seqs), F32)
    )
    hidden_t = silu(hot_t[:16]) * hot_t[16:]
    hh[core * RING + z] = jnp.concatenate([hidden_t, jnp.zeros_like(hidden_t)], axis=1).astype(
        BF16
    )

    def hh_copy(k):
        return remote(
            hh.at[core * RING + z],
            hh.at[core * RING + z],
            hh_send,
            hh_recv,
            along_z(ring(z, k)),
            partner,
        )

    z_copies(FAR_Z, lambda k: hh_copy(k).start())

    half = lax.rem(z, 2)
    rows = lax.div(z, 2)
    slot_own = pair_of(core, p) * 2 + half
    block_own = jnp.int32(0)
    for k in range(CAP):
        block_own = jnp.where(slot_own == k, slots[k], block_own)
    landed(hidx, load_sem.at[5])
    unit = (cold * blocks_here + block_own) * LANES + lax.broadcasted_iota(
        jnp.int32, (LANES, LANES), 0
    )

    def match(c, found):
        return jnp.where(hidx[:, place(c)] == unit, 1.0, found)

    found = lax.fori_loop(
        0, hidx.shape[1] // LANES, match, jnp.zeros((LANES, LANES), F32), unroll=4
    )
    hot_units = lax.dot_general(
        jnp.ones((8, LANES), BF16),
        found.astype(BF16),
        (((1,), (1,)), ((), ())),
        preferred_element_type=F32,
    )[0:1]
    chosen = jnp.sum(
        jnp.where(block_id == block_own, mpad[...], 0).astype(F32), axis=0, keepdims=True
    )
    row = lax.broadcasted_iota(jnp.int32, (16, LANES), 0) + rows * 16
    column = lax.broadcasted_iota(jnp.int32, (16, LANES), 1)
    seq_live = jnp.sum(jnp.where(row == column, chosen, 0.0), axis=1, keepdims=True)
    lv[core] = (seq_live * (1.0 - jnp.minimum(hot_units, 1.0))).astype(BF16)
    lv_copy = remote(lv.at[0], lv.at[0], lv_send, lv_recv, hot, partner)

    @pl.when(core == 0)
    def _():
        lv_copy.start()

    landed(cd, load_sem.at[6])
    for k in range(CAP):
        block = cd[pl.ds(slots[k] * LANES, LANES), :]
        cds[k // 2, :, LANES * (k % 2) : LANES * (k % 2) + LANES] = jnp.transpose(block)

    def cd_copy(k, to):
        return remote(
            cds.at[pair_of(core, to)],
            cdr.at[core, p],
            cd_send,
            cd_recv.at[core],
            in_plane(to),
            partner,
        )

    def start_cd(k, to, sends):
        @pl.when(sends)
        def _():
            cd_copy(k, to).start()

    def s2_copies(group, op, own=None):
        for at in range(Z_FIRST, RING):
            to = lax.rem(pair_of(group, p) + at, RING)
            copy = remote(
                s2.at[group, at - Z_FIRST],
                r2.at[group * RING + z],
                s2_send.at[group],
                r2_recv.at[group],
                along_z(to),
                partner,
            )

            @pl.when(to != z)
            def _():
                op(copy)

            if own is not None:

                @pl.when(to == z)
                def _():
                    own(at - Z_FIRST)

    def sq_copy(group, b):
        to = swap(group, pair_at(z, b))
        return to, remote(
            sq.at[group, b],
            r2.at[group * RING + p],
            sq_send.at[group, b],
            r2_recv.at[group],
            in_plane(jnp.maximum(to, 0)),
            partner,
        )

    piece = half * 4 + rows

    def h3_copy(group, k):
        return remote(
            h3.at[group, piece],
            h3.at[group, piece],
            h3_send.at[group],
            h3_recv.at[group],
            along_z(ring(z, k)),
            partner,
        )

    def fs_copy(k, other, core_to):
        cold_to = lax.rem(x_hi + other, 2) * 2 + core_to
        return remote(
            fs.at[4 * k + cold_to],
            fr.at[2 * k + other],
            fs_send,
            fs_recv,
            in_plane(in_plane_at(k)[0]),
            cold_to,
        )

    @pl.when(core == 0)
    def _():
        pl.semaphore_wait(go, 1)
        for k in LATE_Z:
            hd_copy(k).start()
        plane_copies(FAR_PLANE, start_cd)

    @pl.when(adds)
    def _():
        for group in (1, 0):
            for b in range(Z_FIRST):
                pair = pair_at(z, b)

                @pl.when(pair < PAIRS)
                def _():
                    if group:
                        total = s1[jnp.minimum(pair, PAIRS - 1), b].astype(F32)
                    else:
                        total = jnp.zeros(s1.shape[2:], F32)
                    landed(rb.at[group, b, pl.ds(0, RING - group)], sb_recv.at[group, b])
                    for k in range(group, RING):
                        total = total + rb[group, b, ring(z, k)].astype(F32)
                    sq[group, b] = total.astype(BF16)
                    to, copy = sq_copy(group, b)

                    @pl.when(to != p)
                    def _():
                        copy.start()

                    @pl.when(to == p)
                    def _():
                        r2[group * RING + p] = sq[group, b]

        for group in (1, 0):

            @pl.when(works(group))
            def _():
                if group:
                    total = s1[pair_of(1, p), Z_FIRST:].astype(F32)
                else:
                    total = jnp.zeros((RING - Z_FIRST, *s1.shape[2:]), F32)
                landed(r1.at[group, pl.ds(0, RING - group)], s1_recv.at[group])
                for k in range(group, RING):
                    total = total + r1[group, ring(p, k)].astype(F32)
                s2[group] = total.astype(BF16)

                def own(at):
                    r2[group * RING + z] = s2[group, at]

                s2_copies(group, lambda copy: copy.start(), own)

        pl.semaphore_signal(
            go, inc=1, device_id=(hot, x_hi * 2), device_id_type=MESH
        )

        for k in LATE_Z:
            hd_copy(k).start()
        plane_copies(FAR_PLANE, start_cd)
        cdr[1, p] = cds[pair_of(1, p)]

        remote(lv.at[0], lv.at[0], lv_send, lv_recv, hot, partner).wait_recv()
        for group in (1, 0):

            @pl.when(works(group))
            def _():
                pieces = r2.at[pl.ds(group * RING, RING)]
                landed(pieces.at[pl.ds(0, RING - 1)], r2_recv.at[group])
                both = pieces[0].astype(F32)
                for i in range(1, RING):
                    both = both + pieces[i].astype(F32)
                live = lv[group].astype(F32)
                h3[group, piece] = (silu(both[0]) * both[1] * live).astype(BF16)
                for k in FAR_Z:
                    h3_copy(group, k).start()

        own_piece.wait()
        landed(hdp.at[pl.ds(0, 2 * RING - 1)], hd_recv)
        landed(hh.at[pl.ds(0, 2 * RING - 1)], hh_recv)
        hidden = hh[...].reshape(2 * LANES, LANES)[:, :seqs]
        for q in range(RING):
            down = hdp[:, :, LANES * q : LANES * q + LANES].reshape(2 * LANES, LANES)
            acc[q] = jnp.dot(jnp.transpose(down), hidden, preferred_element_type=F32)

        def await_pair(group):
            @pl.when(works(group))
            def _():
                landed(cdr.at[group, pl.ds(0, RING - group)], cd_recv.at[group])
                landed(h3.at[group, pl.ds(0, RING - 1)], h3_recv.at[group])

        def pair_hidden(group):
            return jnp.concatenate(
                [
                    h3[group, 0:4].reshape(seqs, LANES),
                    h3[group, 4:8].reshape(seqs, LANES),
                ],
                axis=1,
            )

        def pair_term(group, values, to):
            term = lax.dot_general(
                cdr[group, to],
                values,
                (((1,), (1,)), ((), ())),
                preferred_element_type=F32,
            )
            return acc[to] + jnp.where(works(group), term, 0.0)

        await_pair(1)
        values = pair_hidden(1)
        for q in range(RING):
            acc[q] = pair_term(1, values, q)
        await_pair(0)

        values = pair_hidden(0)
        terms = [pair_term(0, values, in_plane_at(k)[0]) for k in (*FAR_PLANE, 0)]
        for k, term in zip((*FAR_PLANE, 0), terms):
            for c in range(4):
                fs[4 * k + c] = jnp.concatenate(
                    [term[32 * c : 32 * c + 16], term[32 * c + 16 : 32 * c + 32]], axis=1
                ).astype(BF16)
            for other, core_to in ((1, 0), (1, 1), (0, 0), (0, 1)):
                if k + other or not core_to:
                    fs_copy(k, other, core_to).start()

        fr[0] = fs[cold]

    @pl.when(adds)
    def _():
        landed = fr.at[pl.ds(1, 2 * RING - 1)]
        pltpu.make_async_copy(landed, landed, fs_recv).wait()

    @pl.when(core == 0)
    def _():
        pltpu.make_async_copy(fr, fr, fs_recv).wait()

    result = fr[0].astype(F32)
    for i in range(1, 2 * RING):
        result = result + fr[i].astype(F32)
    out_ref[0:16, :] = result[:, :seqs].astype(BF16)
    out_ref[16:32, :] = result[:, seqs:].astype(BF16)

    fewer = jnp.logical_and(adds, works(1))
    ends = jnp.logical_or(z == 0, z == RING - 1)

    @pl.when(fewer)
    def _():
        landed(r1.at[0, pl.ds(0, PAIRS - 1)], s1_send)
        landed(cdr.at[0, pl.ds(0, PAIRS - 1)], cd_send)

    @pl.when(jnp.logical_not(fewer))
    def _():
        landed(r1.at[0, pl.ds(0, PAIRS)], s1_send)
        landed(cdr.at[0, pl.ds(0, PAIRS)], cd_send)

    @pl.when(core == 0)
    def _():
        landed(r2.at[pl.ds(0, 14)], sb_send)
        landed(hdp.at[pl.ds(0, RING)], hd_send)
        landed(hh.at[pl.ds(0, RING)], hh_send)
        lv_copy.wait_send()

    @pl.when(adds)
    def _():
        landed(hdp.at[pl.ds(0, RING - 1)], hd_send)
        landed(hh.at[pl.ds(0, RING - 1)], hh_send)

        @pl.when(ends)
        def _():
            landed(r2.at[pl.ds(0, 13)], sb_send)

        @pl.when(jnp.logical_not(ends))
        def _():
            landed(r2.at[pl.ds(0, 12)], sb_send)

        for group in range(2):
            z_first = lax.rem(z + RING - pair_of(group, p), RING) < Z_FIRST

            @pl.when(jnp.logical_and(works(group), z_first))
            def _():
                landed(r2.at[pl.ds(0, RING - Z_FIRST)], s2_send.at[group])

            @pl.when(jnp.logical_and(works(group), jnp.logical_not(z_first)))
            def _():
                landed(r2.at[pl.ds(0, RING - Z_FIRST - 1)], s2_send.at[group])

            @pl.when(works(group))
            def _():
                landed(h3.at[group, pl.ds(0, RING - 1)], h3_send.at[group])

            for b in range(Z_FIRST):
                to, copy = sq_copy(group, b)

                @pl.when(jnp.logical_and(pair_at(z, b) < PAIRS, to != p))
                def _():
                    copy.wait_send()

        landed(fs.at[pl.ds(0, 4 * RING - 1)], fs_send)


def on_device(
    tokens,
    norm_gain,
    hot_gate,
    hot_up,
    hot_down,
    hot_index,
    cold_gate,
    cold_up,
    cold_down,
    block_mask,
):
    seqs, features = tokens.shape
    dma = pltpu.SemaphoreType.DMA
    any_space = pl.BlockSpec(memory_space=pl.ANY)
    return pl.pallas_call(
        kernel,
        out_shape=jax.ShapeDtypeStruct((32, seqs), BF16),
        in_specs=[any_space] * 10,
        out_specs=pl.BlockSpec(memory_space=pltpu.VMEM),
        scratch_shapes=[
            pltpu.VMEM(tokens.shape, BF16),
            pltpu.VMEM((1, features), F32),
            pltpu.VMEM((32, features), BF16),
            pltpu.VMEM((1, hot_index.shape[0]), jnp.int32),
            pltpu.VMEM((2, *cold_gate.shape), BF16),
            pltpu.VMEM(cold_down.shape, BF16),
            pltpu.VMEM(block_mask.shape[::-1], jnp.int32),
            pltpu.VMEM((32, LANES), jnp.int32),
            pltpu.VMEM((PAIRS, RING, 2, 16, LANES), BF16),
            pltpu.VMEM((2, RING, RING - Z_FIRST, 2, 16, LANES), BF16),
            pltpu.VMEM((2, Z_FIRST, RING, 2, 16, LANES), BF16),
            pltpu.VMEM((2, Z_FIRST, 2, 16, LANES), BF16),
            pltpu.VMEM((2, RING - Z_FIRST, 2, 16, LANES), BF16),
            pltpu.VMEM((2 * RING, 2, 16, LANES), BF16),
            pltpu.VMEM((2, RING, 16, LANES), BF16),
            pltpu.VMEM((PAIRS, LANES, 2 * LANES), BF16),
            pltpu.VMEM((2, RING, LANES, 2 * LANES), BF16),
            pltpu.VMEM((2 * RING, 16, RING * LANES), BF16),
            pltpu.VMEM((2 * RING, 16, LANES), BF16),
            pltpu.VMEM((2, 16, LANES), BF16),
            pltpu.VMEM((RING, LANES, seqs), F32),
            pltpu.VMEM((RING * 4, 16, LANES), BF16),
            pltpu.VMEM((2 * RING, 16, LANES), BF16),
            dma((8,)),
            dma,
            dma((2,)),
            dma,
            dma((2, Z_FIRST)),
            dma((2, Z_FIRST)),
            dma((2,)),
            dma((2,)),
            dma((2,)),
            dma((2,)),
            dma,
            dma((2,)),
            dma,
            dma,
            dma,
            dma,
            dma,
            dma,
            pltpu.SemaphoreType.REGULAR,
            dma,
            dma,
        ],
        compiler_params=pltpu.CompilerParams(
            collective_id=0, has_side_effects=True, vmem_limit_bytes=55218 * 1024
        ),
    )(
        tokens,
        norm_gain.reshape(1, -1),
        hot_gate,
        hot_up,
        hot_down,
        hot_index.reshape(1, -1),
        cold_gate,
        cold_up,
        cold_down,
        block_mask.T,
    ).T


def solution(mesh):
    rows = P(("hot", "cold"), None)
    return jax.shard_map(
        on_device,
        mesh=mesh,
        in_specs=(
            P(),
            P(),
            rows,
            rows,
            rows,
            P(),
            P("hot", "cold"),
            P("hot", "cold"),
            P("cold", "hot"),
            P(None, "cold"),
        ),
        out_specs=P(None, ("hot", "cold")),
        check_vma=False,
    )
```

```python
import functools

import jax
import jax.numpy as jnp
from jax import lax
from jax.experimental import pallas as pl
from jax.experimental.pallas import tpu as pltpu
from jax.sharding import PartitionSpec as P

MESH = pl.DeviceIdType.MESH
F32 = jnp.float32
BF16 = jnp.bfloat16
RING = 8
FAR_Z = (4, 3, 5, 2, 6, 1, 7)
NEAR_Z = (2, 6, 1, 7)
BEYOND_Z = (4, 3, 5)
FAR_PLANE = (5, 4, 3, 7, 2, 6, 1)
PAIRS = 7
CAP = 14
LANES = 128
EPS = 1e-05
CHUNK = 1024


def silu(v):
    return v / (1.0 + jnp.exp(-v))


def place(index):
    return pl.ds(pl.multiple_of(index * LANES, LANES), LANES)


def kernel(
    tok_hbm,
    gain_hbm,
    hg_hbm,
    hu_hbm,
    hd_hbm,
    hidx_hbm,
    cg_hbm,
    cu_hbm,
    cd_hbm,
    mask_hbm,
    out_ref,
    tok,
    gain,
    hw,
    hidx,
    cgu,
    cd,
    msk,
    mpad,
    s1,
    r1,
    s2,
    r2,
    h3,
    cds,
    cdr,
    hdp,
    hh,
    lv,
    acc,
    fs,
    fr,
    load_sem,
    plane_send,
    s1_recv,
    s2_send,
    r2_recv,
    h3_send,
    h3_recv,
    cd_recv,
    hd_send,
    hd_recv,
    hh_send,
    hh_recv,
    lv_send,
    lv_recv,
    go,
    zgo,
    xgo,
    fs_send,
    fs_recv,
):
    hot = lax.axis_index("hot")
    cold = lax.axis_index("cold")
    z = lax.div(hot, RING)
    p = lax.rem(hot, RING)
    x_hi = lax.div(cold, 2)
    core = lax.rem(cold, 2)
    adds = core == 1
    partner = x_hi * 2 + 1
    seqs, features = tok.shape
    blocks_here = msk.shape[0]

    def ring(base, k):
        return lax.rem(base + k, RING)

    def in_plane_at(k):
        dy, dx = divmod(k, 2)
        y, x = lax.div(p, 2), lax.rem(p, 2)
        return tuple(
            lax.rem(y + d, 4) * 2 + x + dx * (1 - 2 * x) for d in (dy, 4 - dy)
        )

    def swap(group, place_or_pair):
        return 7 - place_or_pair + group * (2 * place_or_pair - 7)

    def works(group):
        return swap(group, p) < PAIRS

    def pair_of(group, to):
        return jnp.minimum(swap(group, to), PAIRS - 1)

    def remote(src, dst, send, recv, hot_to, cold_to):
        return pltpu.make_async_remote_copy(
            src_ref=src,
            dst_ref=dst,
            send_sem=send,
            recv_sem=recv,
            device_id=(hot_to, cold_to),
            device_id_type=MESH,
        )

    def landed(ref, sem):
        pltpu.make_async_copy(ref, ref, sem).wait()

    def in_plane(to):
        return z * RING + to

    def along_z(to):
        return to * RING + p

    loads = [
        (mask_hbm, msk, 0),
        (tok_hbm, tok, 1),
        (gain_hbm, gain, 2),
        (cg_hbm, cgu.at[0], 3),
        (cu_hbm, cgu.at[1], 3),
        (hg_hbm, hw.at[pl.ds(0, 16)], 4),
        (hu_hbm, hw.at[pl.ds(16, 16)], 4),
        (hidx_hbm, hidx, 5),
        (cd_hbm, cd, 6),
    ]
    for src, dst, sem in loads:
        pltpu.make_async_copy(src, dst, load_sem.at[sem]).start()

    def columns_of(zz):
        return pl.ds(pl.multiple_of(zz * RING * LANES, RING * LANES), RING * LANES)

    own_piece = pltpu.make_async_copy(
        hd_hbm.at[:, columns_of(z)], hdp.at[RING + z], load_sem.at[7]
    )

    @pl.when(adds)
    def _():
        own_piece.start()

    barrier = pltpu.get_barrier_semaphore()

    def greet(hot_to, cold_to):
        pl.semaphore_signal(
            barrier, inc=1, device_id=(hot_to, cold_to), device_id_type=MESH
        )

    other_x = (1 - x_hi) * 2 + 1
    for k in FAR_PLANE:
        greet(in_plane(in_plane_at(k)[0]), partner)
    for k in NEAR_Z:
        greet(along_z(ring(z, k)), partner)

    @pl.when(adds)
    def _():
        for k in (*FAR_PLANE, 0):
            greet(in_plane(in_plane_at(k)[0]), x_hi * 2)
        for k in NEAR_Z:
            greet(along_z(ring(z, k)), x_hi * 2)
        greet(hot, other_x)

    @pl.when(core == 0)
    def _():
        greet(hot, partner)

    landed(msk, load_sem.at[0])
    mpad[...] = jnp.zeros_like(mpad)
    mpad[0:blocks_here, 0:seqs] = msk[...]
    block_id = lax.broadcasted_iota(jnp.int32, mpad.shape, 0)
    lane_id = lax.broadcasted_iota(jnp.int32, mpad.shape, 1)
    active = mpad[...]
    step = 1
    while step < LANES:
        active = jnp.maximum(active, pltpu.roll(active, step, 1))
        step *= 2
    upto = active
    step = 1
    while step < 32:
        upto = upto + jnp.where(block_id >= step, pltpu.roll(upto, step, 0), 0)
        step *= 2
    ahead = upto - active
    rank = jnp.where(active > 0, ahead, upto[31:32] + block_id - ahead)
    order = jnp.sum(jnp.where(rank == lane_id, block_id, 0), axis=0, keepdims=True)
    slots = [order[0, k] for k in range(CAP)]

    landed(tok, load_sem.at[1])
    landed(gain, load_sem.at[2])

    def add_squares(c, total):
        x = tok[:, place(c)].astype(F32)
        return total + x * x

    squares = lax.fori_loop(
        0, features // LANES, add_squares, jnp.zeros((seqs, LANES), F32), unroll=8
    )
    scale = lax.rsqrt(jnp.sum(squares, axis=1, keepdims=True) / features + EPS)
    mine = (tok[:, place(hot)].astype(F32) * scale * gain[:, place(hot)]).astype(BF16)

    landed(cgu, load_sem.at[3])
    for k in range(CAP):
        cols = pl.ds(slots[k] * LANES, LANES)
        both = jnp.concatenate([cgu[0, :, cols], cgu[1, :, cols]], axis=1)
        part = jnp.dot(mine, both, preferred_element_type=F32).astype(BF16)
        for r in range(4):
            at = 2 * r + k % 2
            s1[k // 2, at, 0] = part[16 * r : 16 * r + 16, :LANES]
            s1[k // 2, at, 1] = part[16 * r : 16 * r + 16, LANES:]

    @pl.when(adds)
    def _():
        pl.semaphore_wait(barrier, 24)
        for k in (2, 6):
            for core_to in range(2):
                pl.semaphore_signal(
                    zgo,
                    inc=1,
                    device_id=(along_z(ring(z, k)), x_hi * 2 + core_to),
                    device_id_type=MESH,
                )
        pl.semaphore_signal(xgo, inc=1, device_id=(hot, other_x), device_id_type=MESH)

    @pl.when(core == 0)
    def _():
        pl.semaphore_wait(barrier, 12)

    def plane_copies(order, op):
        for k in (*order, 0):
            to = in_plane_at(k)[0]
            sends = swap(core, to) < PAIRS
            if k == 0:
                sends = jnp.logical_and(sends, core == 0)
            op(k, to, sends)

    def s1_copy(k, to):
        return remote(
            s1.at[pair_of(core, to)],
            r1.at[core * RING + p],
            plane_send,
            s1_recv.at[core],
            in_plane(to),
            partner,
        )

    def start_s1(k, to, sends):
        @pl.when(sends)
        def _():
            s1_copy(k, to).start()

    plane_copies(FAR_PLANE, start_s1)

    def z_copies(order, op):
        for k in order:
            if k:
                op(k)
            else:
                pl.when(core == 0)(lambda: op(0))

    def hd_copy(k):
        to = ring(z, k)
        return remote(
            hd_hbm.at[:, columns_of(to)],
            hdp.at[core * RING + z],
            hd_send,
            hd_recv,
            along_z(to),
            partner,
        )

    z_copies((*NEAR_Z, 0), lambda k: hd_copy(k).start())

    half = lax.rem(z, 2)
    rows = lax.div(z, 2)
    slot_own = pair_of(core, p) * 2 + half
    block_own = jnp.int32(0)
    for k in range(CAP):
        block_own = jnp.where(slot_own == k, slots[k], block_own)
    landed(hidx, load_sem.at[5])
    unit = (cold * blocks_here + block_own) * LANES + lax.broadcasted_iota(
        jnp.int32, (LANES, LANES), 0
    )

    def match(c, found):
        return jnp.where(hidx[:, place(c)] == unit, 1.0, found)

    found = lax.fori_loop(
        0, hidx.shape[1] // LANES, match, jnp.zeros((LANES, LANES), F32), unroll=4
    )
    hot_units = lax.dot_general(
        jnp.ones((8, LANES), BF16),
        found.astype(BF16),
        (((1,), (1,)), ((), ())),
        preferred_element_type=F32,
    )[0:1]
    chosen = jnp.sum(
        jnp.where(block_id == block_own, mpad[...], 0).astype(F32), axis=0, keepdims=True
    )
    row = lax.broadcasted_iota(jnp.int32, (16, LANES), 0) + rows * 16
    column = lax.broadcasted_iota(jnp.int32, (16, LANES), 1)
    seq_live = jnp.sum(jnp.where(row == column, chosen, 0.0), axis=1, keepdims=True)
    lv[core] = (seq_live * (1.0 - jnp.minimum(hot_units, 1.0))).astype(BF16)
    lv_copy = remote(lv.at[0], lv.at[0], lv_send, lv_recv, hot, partner)

    @pl.when(core == 0)
    def _():
        lv_copy.start()

    landed(cd, load_sem.at[6])
    for k in range(CAP):
        block = cd[pl.ds(slots[k] * LANES, LANES), :]
        cds[k // 2, :, LANES * (k % 2) : LANES * (k % 2) + LANES] = jnp.transpose(block)

    pl.semaphore_wait(zgo, 2)
    z_copies(BEYOND_Z, lambda k: hd_copy(k).start())

    landed(hw, load_sem.at[4])

    def hot_chunk(c, total):
        cols = pl.ds(pl.multiple_of(c * CHUNK, CHUNK), CHUNK)
        normed = (tok[:, cols].astype(F32) * scale * gain[:, cols]).astype(BF16)
        return total + lax.dot_general(
            hw[:, cols], normed, (((1,), (1,)), ((), ())), preferred_element_type=F32
        )

    hot_t = lax.fori_loop(
        0, features // CHUNK, hot_chunk, jnp.zeros((32, seqs), F32)
    )
    hidden_t = silu(hot_t[:16]) * hot_t[16:]
    hh[core * RING + z] = jnp.concatenate([hidden_t, jnp.zeros_like(hidden_t)], axis=1).astype(
        BF16
    )

    def hh_copy(k):
        return remote(
            hh.at[core * RING + z],
            hh.at[core * RING + z],
            hh_send,
            hh_recv,
            along_z(ring(z, k)),
            partner,
        )

    z_copies((*FAR_Z, 0), lambda k: hh_copy(k).start())

    def cd_copy(k, to):
        return remote(
            cds.at[pair_of(core, to)],
            cdr.at[core, p],
            plane_send,
            cd_recv.at[core],
            in_plane(to),
            partner,
        )

    def start_cd(k, to, sends):
        @pl.when(sends)
        def _():
            cd_copy(k, to).start()

    def s2_copy(group, k):
        to = ring(z, k)
        return remote(
            s2.at[group, to],
            r2.at[group * RING + z],
            s2_send,
            r2_recv.at[group],
            along_z(to),
            partner,
        )

    piece = half * 4 + rows

    def h3_copy(group, k):
        return remote(
            h3.at[group, piece],
            h3.at[group, piece],
            h3_send,
            h3_recv.at[group],
            along_z(ring(z, k)),
            partner,
        )

    def fs_copy(k, other, core_to):
        cold_to = lax.rem(x_hi + other, 2) * 2 + core_to
        return remote(
            fs.at[4 * k + cold_to],
            fr.at[2 * k + other],
            fs_send,
            fs_recv,
            in_plane(in_plane_at(k)[0]),
            cold_to,
        )

    @pl.when(core == 0)
    def _():
        pl.semaphore_wait(go, 1)
        plane_copies(FAR_PLANE, start_cd)

    @pl.when(adds)
    def _():
        for group in (1, 0):

            @pl.when(works(group))
            def _():
                if group:
                    total = s1[pair_of(1, p)].astype(F32)
                else:
                    total = jnp.zeros(s1.shape[1:], F32)
                base = group * RING
                landed(r1.at[pl.ds(base, RING - group)], s1_recv.at[group])
                for k in range(group, RING):
                    total = total + r1[base + ring(p, k)].astype(F32)
                s2[group] = total.astype(BF16)
                for k in FAR_Z:
                    s2_copy(group, k).start()
                r2[base + z] = s2[group, z]

        pl.semaphore_signal(
            go, inc=1, device_id=(hot, x_hi * 2), device_id_type=MESH
        )

        plane_copies(FAR_PLANE, start_cd)
        cdr[1, p] = cds[pair_of(1, p)]

        remote(lv.at[0], lv.at[0], lv_send, lv_recv, hot, partner).wait_recv()
        for group in (1, 0):

            @pl.when(works(group))
            def _():
                pieces = r2.at[pl.ds(group * RING, RING)]
                landed(pieces.at[pl.ds(0, RING - 1)], r2_recv.at[group])
                both = pieces[0].astype(F32)
                for i in range(1, RING):
                    both = both + pieces[i].astype(F32)
                live = lv[group].astype(F32)
                h3[group, piece] = (silu(both[0]) * both[1] * live).astype(BF16)
                for k in FAR_Z:
                    h3_copy(group, k).start()

        own_piece.wait()
        landed(hdp.at[pl.ds(0, 2 * RING - 1)], hd_recv)
        landed(hh.at[pl.ds(0, 2 * RING - 1)], hh_recv)
        hidden = hh[...].reshape(2 * LANES, LANES)[:, :seqs]
        for q in range(RING):
            down = hdp[:, :, LANES * q : LANES * q + LANES].reshape(2 * LANES, LANES)
            acc[q] = jnp.dot(jnp.transpose(down), hidden, preferred_element_type=F32)

        pl.semaphore_wait(xgo, 1)

        def await_pair(group):
            @pl.when(works(group))
            def _():
                landed(cdr.at[group, pl.ds(0, RING - group)], cd_recv.at[group])
                landed(h3.at[group, pl.ds(0, RING - 1)], h3_recv.at[group])

        def pair_hidden(group):
            return jnp.concatenate(
                [
                    h3[group, 0:4].reshape(seqs, LANES),
                    h3[group, 4:8].reshape(seqs, LANES),
                ],
                axis=1,
            )

        def pair_term(group, values, to):
            term = lax.dot_general(
                cdr[group, to],
                values,
                (((1,), (1,)), ((), ())),
                preferred_element_type=F32,
            )
            return acc[to] + jnp.where(works(group), term, 0.0)

        await_pair(1)
        values = pair_hidden(1)
        for q in range(RING):
            acc[q] = pair_term(1, values, q)
        await_pair(0)

        values = pair_hidden(0)
        terms = [pair_term(0, values, in_plane_at(k)[0]) for k in (*FAR_PLANE, 0)]
        for k, term in zip((*FAR_PLANE, 0), terms):
            for c in range(4):
                fs[4 * k + c] = jnp.concatenate(
                    [term[32 * c : 32 * c + 16], term[32 * c + 16 : 32 * c + 32]], axis=1
                ).astype(BF16)
            for other, core_to in ((1, 0), (1, 1), (0, 0), (0, 1)):
                if k + other or not core_to:
                    fs_copy(k, other, core_to).start()

        fr[0] = fs[cold]

    @pl.when(adds)
    def _():
        landed = fr.at[pl.ds(1, 2 * RING - 1)]
        pltpu.make_async_copy(landed, landed, fs_recv).wait()

    @pl.when(core == 0)
    def _():
        pltpu.make_async_copy(fr, fr, fs_recv).wait()

    result = fr[0].astype(F32)
    for i in range(1, 2 * RING):
        result = result + fr[i].astype(F32)
    out_ref[0:16, :] = result[:, :seqs].astype(BF16)
    out_ref[16:32, :] = result[:, seqs:].astype(BF16)

    fewer = jnp.logical_and(adds, works(1))

    @pl.when(fewer)
    def _():
        landed(r1.at[pl.ds(0, 2 * PAIRS - 2)], plane_send)

    @pl.when(jnp.logical_not(fewer))
    def _():
        landed(r1.at[pl.ds(0, 2 * PAIRS)], plane_send)

    @pl.when(core == 0)
    def _():
        landed(hdp.at[pl.ds(0, RING)], hd_send)
        landed(hh.at[pl.ds(0, RING)], hh_send)
        lv_copy.wait_send()

    @pl.when(adds)
    def _():
        landed(hdp.at[pl.ds(0, RING - 1)], hd_send)
        landed(hh.at[pl.ds(0, RING - 1)], hh_send)
        landed(fs.at[pl.ds(0, 4 * RING - 1)], fs_send)
        both_groups = jnp.logical_and(works(0), works(1))

        @pl.when(both_groups)
        def _():
            landed(r2.at[pl.ds(0, 2 * RING - 2)], s2_send)
            landed(hh.at[pl.ds(0, 2 * RING - 2)], h3_send)

        @pl.when(jnp.logical_not(both_groups))
        def _():
            landed(r2.at[pl.ds(0, RING - 1)], s2_send)
            landed(hh.at[pl.ds(0, RING - 1)], h3_send)


def on_device(
    tokens,
    norm_gain,
    hot_gate,
    hot_up,
    hot_down,
    hot_index,
    cold_gate,
    cold_up,
    cold_down,
    block_mask,
):
    seqs, features = tokens.shape
    dma = pltpu.SemaphoreType.DMA
    any_space = pl.BlockSpec(memory_space=pl.ANY)
    return pl.pallas_call(
        kernel,
        out_shape=jax.ShapeDtypeStruct((32, seqs), BF16),
        in_specs=[any_space] * 10,
        out_specs=pl.BlockSpec(memory_space=pltpu.VMEM),
        scratch_shapes=[
            pltpu.VMEM(tokens.shape, BF16),
            pltpu.VMEM((1, features), F32),
            pltpu.VMEM((32, features), BF16),
            pltpu.VMEM((1, hot_index.shape[0]), jnp.int32),
            pltpu.VMEM((2, *cold_gate.shape), BF16),
            pltpu.VMEM(cold_down.shape, BF16),
            pltpu.VMEM(block_mask.shape[::-1], jnp.int32),
            pltpu.VMEM((32, LANES), jnp.int32),
            pltpu.VMEM((PAIRS, RING, 2, 16, LANES), BF16),
            pltpu.VMEM((2 * RING, RING, 2, 16, LANES), BF16),
            pltpu.VMEM((2, RING, 2, 16, LANES), BF16),
            pltpu.VMEM((2 * RING, 2, 16, LANES), BF16),
            pltpu.VMEM((2, RING, 16, LANES), BF16),
            pltpu.VMEM((PAIRS, LANES, 2 * LANES), BF16),
            pltpu.VMEM((2, RING, LANES, 2 * LANES), BF16),
            pltpu.VMEM((2 * RING, 16, RING * LANES), BF16),
            pltpu.VMEM((2 * RING, 16, LANES), BF16),
            pltpu.VMEM((2, 16, LANES), BF16),
            pltpu.VMEM((RING, LANES, seqs), F32),
            pltpu.VMEM((RING * 4, 16, LANES), BF16),
            pltpu.VMEM((2 * RING, 16, LANES), BF16),
            dma((8,)),
            dma,
            dma((2,)),
            dma,
            dma((2,)),
            dma,
            dma((2,)),
            dma((2,)),
            dma,
            dma,
            dma,
            dma,
            dma,
            dma,
            pltpu.SemaphoreType.REGULAR,
            pltpu.SemaphoreType.REGULAR,
            pltpu.SemaphoreType.REGULAR,
            dma,
            dma,
        ],
        compiler_params=pltpu.CompilerParams(
            collective_id=0, has_side_effects=True, vmem_limit_bytes=55218 * 1024
        ),
    )(
        tokens,
        norm_gain.reshape(1, -1),
        hot_gate,
        hot_up,
        hot_down,
        hot_index.reshape(1, -1),
        cold_gate,
        cold_up,
        cold_down,
        block_mask.T,
    ).T


def solution(mesh):
    rows = P(("hot", "cold"), None)
    return jax.shard_map(
        on_device,
        mesh=mesh,
        in_specs=(
            P(),
            P(),
            rows,
            rows,
            rows,
            P(),
            P("hot", "cold"),
            P("hot", "cold"),
            P("cold", "hot"),
            P(None, "cold"),
        ),
        out_specs=P(None, ("hot", "cold")),
        check_vma=False,
    )
```

```python
import functools

import jax
import jax.numpy as jnp
from jax import lax
from jax.experimental import pallas as pl
from jax.experimental.pallas import tpu as pltpu
from jax.sharding import PartitionSpec as P

MESH = pl.DeviceIdType.MESH
F32 = jnp.float32
BF16 = jnp.bfloat16
RING = 8
FAR_Z = (4, 3, 5, 2, 6, 1, 7)
NEAR_Z = (2, 6, 1, 7)
BEYOND_Z = (4, 3, 5)
FAR_PLANE = (5, 4, 3, 7, 2, 6, 1)
PAIRS = 7
CAP = 14
LANES = 128
EPS = 1e-05
CHUNK = 1024


def silu(v):
    return v / (1.0 + jnp.exp(-v))


def place(index):
    return pl.ds(pl.multiple_of(index * LANES, LANES), LANES)


def kernel(
    tok_hbm,
    gain_hbm,
    hg_hbm,
    hu_hbm,
    hd_hbm,
    hidx_hbm,
    cg_hbm,
    cu_hbm,
    cd_hbm,
    mask_hbm,
    out_ref,
    tok,
    gain,
    hw,
    hidx,
    cgu,
    cd,
    msk,
    mpad,
    s1,
    r1,
    s2,
    r2,
    h3,
    cds,
    cdr,
    hdp,
    hh,
    lv,
    acc,
    fs,
    fr,
    load_sem,
    plane_send,
    s1_recv,
    s2_send,
    r2_recv,
    h3_send,
    h3_recv,
    cd_recv,
    hd_send,
    hd_recv,
    hh_send,
    hh_recv,
    lv_send,
    lv_recv,
    go,
    zgo,
    xgo,
    fs_send,
    fs_recv,
):
    hot = lax.axis_index("hot")
    cold = lax.axis_index("cold")
    z = lax.div(hot, RING)
    p = lax.rem(hot, RING)
    x_hi = lax.div(cold, 2)
    core = lax.rem(cold, 2)
    adds = core == 1
    partner = x_hi * 2 + 1
    seqs, features = tok.shape
    blocks_here = msk.shape[0]

    def ring(base, k):
        return lax.rem(base + k, RING)

    def in_plane_at(k):
        dy, dx = divmod(k, 2)
        y, x = lax.div(p, 2), lax.rem(p, 2)
        return tuple(
            lax.rem(y + d, 4) * 2 + x + dx * (1 - 2 * x) for d in (dy, 4 - dy)
        )

    def swap(group, place_or_pair):
        return 7 - place_or_pair + group * (2 * place_or_pair - 7)

    def works(group):
        return swap(group, p) < PAIRS

    def pair_of(group, to):
        return jnp.minimum(swap(group, to), PAIRS - 1)

    def remote(src, dst, send, recv, hot_to, cold_to):
        return pltpu.make_async_remote_copy(
            src_ref=src,
            dst_ref=dst,
            send_sem=send,
            recv_sem=recv,
            device_id=(hot_to, cold_to),
            device_id_type=MESH,
        )

    def landed(ref, sem):
        pltpu.make_async_copy(ref, ref, sem).wait()

    def in_plane(to):
        return z * RING + to

    def along_z(to):
        return to * RING + p

    loads = [
        (mask_hbm, msk, 0),
        (tok_hbm, tok, 1),
        (gain_hbm, gain, 2),
        (cg_hbm, cgu.at[0], 3),
        (cu_hbm, cgu.at[1], 3),
        (hg_hbm, hw.at[pl.ds(0, 16)], 4),
        (hu_hbm, hw.at[pl.ds(16, 16)], 4),
        (hidx_hbm, hidx, 5),
        (cd_hbm, cd, 6),
    ]

    def start_loads(some):
        for src, dst, sem in some:
            pltpu.make_async_copy(src, dst, load_sem.at[sem]).start()

    start_loads(loads[:5])

    def columns_of(zz):
        return pl.ds(pl.multiple_of(zz * RING * LANES, RING * LANES), RING * LANES)

    own_piece = pltpu.make_async_copy(
        hd_hbm.at[:, columns_of(z)], hdp.at[RING + z], load_sem.at[7]
    )

    barrier = pltpu.get_barrier_semaphore()

    def greet(hot_to, cold_to):
        pl.semaphore_signal(
            barrier, inc=1, device_id=(hot_to, cold_to), device_id_type=MESH
        )

    other_x = (1 - x_hi) * 2 + 1
    for k in FAR_PLANE:
        greet(in_plane(in_plane_at(k)[0]), partner)
    for k in NEAR_Z:
        greet(along_z(ring(z, k)), partner)

    @pl.when(adds)
    def _():
        for k in (*FAR_PLANE, 0):
            greet(in_plane(in_plane_at(k)[0]), x_hi * 2)
        for k in NEAR_Z:
            greet(along_z(ring(z, k)), x_hi * 2)
        greet(hot, other_x)

    @pl.when(core == 0)
    def _():
        greet(hot, partner)

    landed(msk, load_sem.at[0])
    mpad[...] = jnp.zeros_like(mpad)
    mpad[0:blocks_here, 0:seqs] = msk[...]
    block_id = lax.broadcasted_iota(jnp.int32, mpad.shape, 0)
    lane_id = lax.broadcasted_iota(jnp.int32, mpad.shape, 1)
    active = jnp.broadcast_to(jnp.max(mpad[...], axis=1, keepdims=True), mpad.shape)
    upto = active
    step = 1
    while step < 32:
        upto = upto + jnp.where(block_id >= step, pltpu.roll(upto, step, 0), 0)
        step *= 2
    ahead = upto - active
    rank = jnp.where(active > 0, ahead, upto[31:32] + block_id - ahead)
    order = jnp.sum(jnp.where(rank == lane_id, block_id, 0), axis=0, keepdims=True)
    slots = [order[0, k] for k in range(CAP)]

    landed(tok, load_sem.at[1])
    landed(gain, load_sem.at[2])

    def add_squares(c, total):
        x = tok[:, place(c)].astype(F32)
        return total + x * x

    squares = lax.fori_loop(
        0, features // LANES, add_squares, jnp.zeros((seqs, LANES), F32), unroll=32
    )
    scale = lax.rsqrt(jnp.sum(squares, axis=1, keepdims=True) / features + EPS)
    mine = (tok[:, place(hot)].astype(F32) * scale * gain[:, place(hot)]).astype(BF16)

    landed(cgu, load_sem.at[3])
    start_loads(loads[5:])

    @pl.when(adds)
    def _():
        own_piece.start()

    for k in range(CAP):
        cols = pl.ds(slots[k] * LANES, LANES)
        both = jnp.concatenate([cgu[0, :, cols], cgu[1, :, cols]], axis=1)
        part = jnp.dot(mine, both, preferred_element_type=F32).astype(BF16)
        for r in range(4):
            at = 2 * r + k % 2
            s1[k // 2, at, 0] = part[16 * r : 16 * r + 16, :LANES]
            s1[k // 2, at, 1] = part[16 * r : 16 * r + 16, LANES:]

    @pl.when(adds)
    def _():
        pl.semaphore_wait(barrier, 24)
        for k in (2, 6):
            for core_to in range(2):
                pl.semaphore_signal(
                    zgo,
                    inc=1,
                    device_id=(along_z(ring(z, k)), x_hi * 2 + core_to),
                    device_id_type=MESH,
                )
        pl.semaphore_signal(xgo, inc=1, device_id=(hot, other_x), device_id_type=MESH)

    @pl.when(core == 0)
    def _():
        pl.semaphore_wait(barrier, 12)

    def plane_copies(order, op):
        for k in (*order, 0):
            to = in_plane_at(k)[0]
            sends = swap(core, to) < PAIRS
            if k == 0:
                sends = jnp.logical_and(sends, core == 0)
            op(k, to, sends)

    def s1_copy(k, to):
        return remote(
            s1.at[pair_of(core, to)],
            r1.at[core * RING + p],
            plane_send,
            s1_recv.at[core],
            in_plane(to),
            partner,
        )

    def start_s1(k, to, sends):
        @pl.when(sends)
        def _():
            s1_copy(k, to).start()

    plane_copies(FAR_PLANE, start_s1)

    def z_copies(order, op):
        for k in order:
            if k:
                op(k)
            else:
                pl.when(core == 0)(lambda: op(0))

    def hd_copy(k):
        to = ring(z, k)
        return remote(
            hd_hbm.at[:, columns_of(to)],
            hdp.at[core * RING + z],
            hd_send,
            hd_recv,
            along_z(to),
            partner,
        )

    z_copies((*NEAR_Z, 0), lambda k: hd_copy(k).start())

    half = lax.rem(z, 2)
    rows = lax.div(z, 2)
    slot_own = pair_of(core, p) * 2 + half
    block_own = jnp.int32(0)
    for k in range(CAP):
        block_own = jnp.where(slot_own == k, slots[k], block_own)
    landed(hidx, load_sem.at[5])
    unit = (cold * blocks_here + block_own) * LANES + lax.broadcasted_iota(
        jnp.int32, (LANES, LANES), 0
    )

    def match(c, found):
        return jnp.where(hidx[:, place(c)] == unit, 1.0, found)

    found = lax.fori_loop(
        0, hidx.shape[1] // LANES, match, jnp.zeros((LANES, LANES), F32), unroll=4
    )
    hot_units = lax.dot_general(
        jnp.ones((8, LANES), BF16),
        found.astype(BF16),
        (((1,), (1,)), ((), ())),
        preferred_element_type=F32,
    )[0:1]
    chosen = jnp.sum(
        jnp.where(block_id == block_own, mpad[...], 0).astype(F32), axis=0, keepdims=True
    )
    row = lax.broadcasted_iota(jnp.int32, (16, LANES), 0) + rows * 16
    column = lax.broadcasted_iota(jnp.int32, (16, LANES), 1)
    seq_live = jnp.sum(jnp.where(row == column, chosen, 0.0), axis=1, keepdims=True)
    lv[core] = (seq_live * (1.0 - jnp.minimum(hot_units, 1.0))).astype(BF16)
    lv_copy = remote(lv.at[0], lv.at[0], lv_send, lv_recv, hot, partner)

    @pl.when(core == 0)
    def _():
        lv_copy.start()

    landed(cd, load_sem.at[6])
    for k in range(CAP):
        block = cd[pl.ds(slots[k] * LANES, LANES), :]
        cds[k // 2, :, LANES * (k % 2) : LANES * (k % 2) + LANES] = jnp.transpose(block)

    pl.semaphore_wait(zgo, 2)
    z_copies(BEYOND_Z, lambda k: hd_copy(k).start())

    landed(hw, load_sem.at[4])

    def hot_chunk(c, total):
        cols = pl.ds(pl.multiple_of(c * CHUNK, CHUNK), CHUNK)
        normed = (tok[:, cols].astype(F32) * scale * gain[:, cols]).astype(BF16)
        return total + lax.dot_general(
            hw[:, cols], normed, (((1,), (1,)), ((), ())), preferred_element_type=F32
        )

    hot_t = lax.fori_loop(
        0, features // CHUNK, hot_chunk, jnp.zeros((32, seqs), F32)
    )
    hidden_t = silu(hot_t[:16]) * hot_t[16:]
    hh[core * RING + z] = jnp.concatenate([hidden_t, jnp.zeros_like(hidden_t)], axis=1).astype(
        BF16
    )

    def hh_copy(k):
        return remote(
            hh.at[core * RING + z],
            hh.at[core * RING + z],
            hh_send,
            hh_recv,
            along_z(ring(z, k)),
            partner,
        )

    z_copies((*FAR_Z, 0), lambda k: hh_copy(k).start())

    def cd_copy(k, to):
        return remote(
            cds.at[pair_of(core, to)],
            cdr.at[core, p],
            plane_send,
            cd_recv.at[core],
            in_plane(to),
            partner,
        )

    def start_cd(k, to, sends):
        @pl.when(sends)
        def _():
            cd_copy(k, to).start()

    def s2_copy(group, k):
        to = ring(z, k)
        return remote(
            s2.at[group, to],
            r2.at[group * RING + z],
            s2_send,
            r2_recv.at[group],
            along_z(to),
            partner,
        )

    piece = half * 4 + rows

    def h3_copy(group, k):
        return remote(
            h3.at[group, piece],
            h3.at[group, piece],
            h3_send,
            h3_recv.at[group],
            along_z(ring(z, k)),
            partner,
        )

    def fs_copy(to, x_to, core_to):
        dy = lax.rem(to // 2 + 4 - lax.div(p, 2), 4)
        dx = lax.rem(to + p, 2)
        dc = lax.rem(x_to + x_hi, 2)
        return remote(
            fs.at[4 * to + 2 * x_to + core_to],
            fr.at[2 * (2 * dy + dx) + dc],
            fs_send,
            fs_recv,
            in_plane(to),
            2 * x_to + core_to,
        )

    @pl.when(core == 0)
    def _():
        pl.semaphore_wait(go, 1)
        plane_copies(FAR_PLANE, start_cd)

    @pl.when(adds)
    def _():
        for group in (1, 0):

            @pl.when(works(group))
            def _():
                if group:
                    total = s1[pair_of(1, p)].astype(F32)
                else:
                    total = jnp.zeros(s1.shape[1:], F32)
                base = group * RING
                landed(r1.at[pl.ds(base, RING - group)], s1_recv.at[group])
                for k in range(group, RING):
                    total = total + r1[base + ring(p, k)].astype(F32)
                s2[group] = total.astype(BF16)
                for k in FAR_Z:
                    s2_copy(group, k).start()
                r2[base + z] = s2[group, z]

        pl.semaphore_signal(
            go, inc=1, device_id=(hot, x_hi * 2), device_id_type=MESH
        )

        plane_copies(FAR_PLANE, start_cd)
        cdr[1, p] = cds[pair_of(1, p)]

        remote(lv.at[0], lv.at[0], lv_send, lv_recv, hot, partner).wait_recv()
        for group in (1, 0):

            @pl.when(works(group))
            def _():
                pieces = r2.at[pl.ds(group * RING, RING)]
                landed(pieces.at[pl.ds(0, RING - 1)], r2_recv.at[group])
                both = pieces[0].astype(F32)
                for i in range(1, RING):
                    both = both + pieces[i].astype(F32)
                live = lv[group].astype(F32)
                h3[group, piece] = (silu(both[0]) * both[1] * live).astype(BF16)
                for k in FAR_Z:
                    h3_copy(group, k).start()

        own_piece.wait()
        landed(hdp.at[pl.ds(0, 2 * RING - 1)], hd_recv)
        landed(hh.at[pl.ds(0, 2 * RING - 1)], hh_recv)
        hidden = hh[...].reshape(2 * LANES, LANES)[:, :seqs]
        for q in range(RING):
            down = hdp[:, :, LANES * q : LANES * q + LANES].reshape(2 * LANES, LANES)
            acc[q] = jnp.dot(jnp.transpose(down), hidden, preferred_element_type=F32)

        pl.semaphore_wait(xgo, 1)

        def await_pair(group):
            @pl.when(works(group))
            def _():
                landed(cdr.at[group, pl.ds(0, RING - group)], cd_recv.at[group])
                landed(h3.at[group, pl.ds(0, RING - 1)], h3_recv.at[group])

        def pair_hidden(group):
            return jnp.concatenate(
                [
                    h3[group, 0:4].reshape(seqs, LANES),
                    h3[group, 4:8].reshape(seqs, LANES),
                ],
                axis=1,
            )

        def pair_term(group, values, to):
            term = lax.dot_general(
                cdr[group, to],
                values,
                (((1,), (1,)), ((), ())),
                preferred_element_type=F32,
            )
            return acc[to] + jnp.where(works(group), term, 0.0)

        await_pair(1)
        values = pair_hidden(1)
        for q in range(RING):
            acc[q] = pair_term(1, values, q)
        await_pair(0)

        values = pair_hidden(0)
        terms = [pair_term(0, values, to) for to in range(RING)]
        for to, term in enumerate(terms):
            for c in range(4):
                fs[4 * to + c] = jnp.concatenate(
                    [term[32 * c : 32 * c + 16], term[32 * c + 16 : 32 * c + 32]], axis=1
                ).astype(BF16)
            for x_to, core_to in ((0, 1), (0, 0), (1, 1), (1, 0)):
                copy = fs_copy(to, x_to, core_to)
                if core_to:
                    own = jnp.logical_and(to == p, x_hi == x_to)
                    pl.when(jnp.logical_not(own))(copy.start)
                else:
                    copy.start()

        fr[0] = fs[4 * p + cold]

    @pl.when(adds)
    def _():
        landed = fr.at[pl.ds(1, 2 * RING - 1)]
        pltpu.make_async_copy(landed, landed, fs_recv).wait()

    @pl.when(core == 0)
    def _():
        pltpu.make_async_copy(fr, fr, fs_recv).wait()

    result = fr[0].astype(F32)
    for i in range(1, 2 * RING):
        result = result + fr[i].astype(F32)
    out_ref[0:16, :] = result[:, :seqs].astype(BF16)
    out_ref[16:32, :] = result[:, seqs:].astype(BF16)

    fewer = jnp.logical_and(adds, works(1))

    @pl.when(fewer)
    def _():
        landed(r1.at[pl.ds(0, 2 * PAIRS - 2)], plane_send)

    @pl.when(jnp.logical_not(fewer))
    def _():
        landed(r1.at[pl.ds(0, 2 * PAIRS)], plane_send)

    @pl.when(core == 0)
    def _():
        landed(hdp.at[pl.ds(0, RING)], hd_send)
        landed(hh.at[pl.ds(0, RING)], hh_send)
        lv_copy.wait_send()

    @pl.when(adds)
    def _():
        landed(hdp.at[pl.ds(0, RING - 1)], hd_send)
        landed(hh.at[pl.ds(0, RING - 1)], hh_send)
        landed(fs.at[pl.ds(0, 4 * RING - 1)], fs_send)
        both_groups = jnp.logical_and(works(0), works(1))

        @pl.when(both_groups)
        def _():
            landed(r2.at[pl.ds(0, 2 * RING - 2)], s2_send)
            landed(hh.at[pl.ds(0, 2 * RING - 2)], h3_send)

        @pl.when(jnp.logical_not(both_groups))
        def _():
            landed(r2.at[pl.ds(0, RING - 1)], s2_send)
            landed(hh.at[pl.ds(0, RING - 1)], h3_send)


def on_device(
    tokens,
    norm_gain,
    hot_gate,
    hot_up,
    hot_down,
    hot_index,
    cold_gate,
    cold_up,
    cold_down,
    block_mask,
):
    seqs, features = tokens.shape
    dma = pltpu.SemaphoreType.DMA
    any_space = pl.BlockSpec(memory_space=pl.ANY)
    return pl.pallas_call(
        kernel,
        out_shape=jax.ShapeDtypeStruct((32, seqs), BF16),
        in_specs=[any_space] * 10,
        out_specs=pl.BlockSpec(memory_space=pltpu.VMEM),
        scratch_shapes=[
            pltpu.VMEM(tokens.shape, BF16),
            pltpu.VMEM((1, features), F32),
            pltpu.VMEM((32, features), BF16),
            pltpu.VMEM((1, hot_index.shape[0]), jnp.int32),
            pltpu.VMEM((2, *cold_gate.shape), BF16),
            pltpu.VMEM(cold_down.shape, BF16),
            pltpu.VMEM(block_mask.shape[::-1], jnp.int32),
            pltpu.VMEM((32, LANES), jnp.int32),
            pltpu.VMEM((PAIRS, RING, 2, 16, LANES), BF16),
            pltpu.VMEM((2 * RING, RING, 2, 16, LANES), BF16),
            pltpu.VMEM((2, RING, 2, 16, LANES), BF16),
            pltpu.VMEM((2 * RING, 2, 16, LANES), BF16),
            pltpu.VMEM((2, RING, 16, LANES), BF16),
            pltpu.VMEM((PAIRS, LANES, 2 * LANES), BF16),
            pltpu.VMEM((2, RING, LANES, 2 * LANES), BF16),
            pltpu.VMEM((2 * RING, 16, RING * LANES), BF16),
            pltpu.VMEM((2 * RING, 16, LANES), BF16),
            pltpu.VMEM((2, 16, LANES), BF16),
            pltpu.VMEM((RING, LANES, seqs), F32),
            pltpu.VMEM((RING * 4, 16, LANES), BF16),
            pltpu.VMEM((2 * RING, 16, LANES), BF16),
            dma((8,)),
            dma,
            dma((2,)),
            dma,
            dma((2,)),
            dma,
            dma((2,)),
            dma((2,)),
            dma,
            dma,
            dma,
            dma,
            dma,
            dma,
            pltpu.SemaphoreType.REGULAR,
            pltpu.SemaphoreType.REGULAR,
            pltpu.SemaphoreType.REGULAR,
            dma,
            dma,
        ],
        compiler_params=pltpu.CompilerParams(
            collective_id=0, has_side_effects=True, vmem_limit_bytes=55218 * 1024
        ),
    )(
        tokens,
        norm_gain.reshape(1, -1),
        hot_gate,
        hot_up,
        hot_down,
        hot_index.reshape(1, -1),
        cold_gate,
        cold_up,
        cold_down,
        block_mask.T,
    ).T


def solution(mesh):
    rows = P(("hot", "cold"), None)
    return jax.shard_map(
        on_device,
        mesh=mesh,
        in_specs=(
            P(),
            P(),
            rows,
            rows,
            rows,
            P(),
            P("hot", "cold"),
            P("hot", "cold"),
            P("cold", "hot"),
            P(None, "cold"),
        ),
        out_specs=P(None, ("hot", "cold")),
        check_vma=False,
    )
```

```python
import functools

import jax
import jax.numpy as jnp
from jax import lax
from jax.experimental import pallas as pl
from jax.experimental.pallas import tpu as pltpu
from jax.sharding import PartitionSpec as P

MESH = pl.DeviceIdType.MESH
F32 = jnp.float32
BF16 = jnp.bfloat16
RING = 8
FAR_Z = (4, 3, 5, 2, 6, 1, 7)
NEAR_Z = (2, 6, 1, 7)
BEYOND_Z = (4, 3, 5)
FAR_PLANE = (5, 4, 3, 7, 2, 6, 1)
PAIRS = 7
CAP = 14
LANES = 128
EPS = 1e-05
CHUNK = 1024


def silu(v):
    return v / (1.0 + jnp.exp(-v))


def place(index):
    return pl.ds(pl.multiple_of(index * LANES, LANES), LANES)


def kernel(
    tok_hbm,
    gain_hbm,
    hg_hbm,
    hu_hbm,
    hd_hbm,
    hidx_hbm,
    cg_hbm,
    cu_hbm,
    cd_hbm,
    mask_hbm,
    out_ref,
    tok,
    gain,
    hw,
    hidx,
    cgu,
    cd,
    msk,
    mpad,
    s1,
    r1,
    s2,
    r2,
    h3,
    cds,
    cdr,
    hdp,
    hh,
    lv,
    acc,
    fs,
    fr,
    load_sem,
    plane_send,
    s1_recv,
    s2_send,
    r2_recv,
    h3_send,
    h3_recv,
    cd_recv,
    hd_send,
    hd_recv,
    hh_send,
    hh_recv,
    lv_send,
    lv_recv,
    go,
    zgo,
    xgo,
    fs_send,
    fs_recv,
):
    hot = lax.axis_index("hot")
    cold = lax.axis_index("cold")
    z = lax.div(hot, RING)
    p = lax.rem(hot, RING)
    x_hi = lax.div(cold, 2)
    core = lax.rem(cold, 2)
    adds = core == 1
    partner = x_hi * 2 + 1
    seqs, features = tok.shape
    blocks_here = msk.shape[0]

    def ring(base, k):
        return lax.rem(base + k, RING)

    def in_plane_at(k):
        dy, dx = divmod(k, 2)
        y, x = lax.div(p, 2), lax.rem(p, 2)
        return tuple(
            lax.rem(y + d, 4) * 2 + x + dx * (1 - 2 * x) for d in (dy, 4 - dy)
        )

    def swap(group, place_or_pair):
        return 7 - place_or_pair + group * (2 * place_or_pair - 7)

    def works(group):
        return swap(group, p) < PAIRS

    def pair_of(group, to):
        return jnp.minimum(swap(group, to), PAIRS - 1)

    def remote(src, dst, send, recv, hot_to, cold_to):
        return pltpu.make_async_remote_copy(
            src_ref=src,
            dst_ref=dst,
            send_sem=send,
            recv_sem=recv,
            device_id=(hot_to, cold_to),
            device_id_type=MESH,
        )

    def landed(ref, sem):
        pltpu.make_async_copy(ref, ref, sem).wait()

    def in_plane(to):
        return z * RING + to

    def along_z(to):
        return to * RING + p

    loads = [
        (mask_hbm, msk, 0),
        (tok_hbm, tok, 1),
        (gain_hbm, gain, 2),
        (cg_hbm, cgu.at[0], 3),
        (cu_hbm, cgu.at[1], 3),
        (hg_hbm, hw.at[pl.ds(0, 16)], 4),
        (hu_hbm, hw.at[pl.ds(16, 16)], 4),
        (hidx_hbm, hidx, 5),
        (cd_hbm, cd, 6),
    ]

    def start_loads(some):
        for src, dst, sem in some:
            pltpu.make_async_copy(src, dst, load_sem.at[sem]).start()

    start_loads(loads[:5])

    def columns_of(zz):
        return pl.ds(pl.multiple_of(zz * RING * LANES, RING * LANES), RING * LANES)

    own_piece = pltpu.make_async_copy(
        hd_hbm.at[:, columns_of(z)], hdp.at[RING + z], load_sem.at[7]
    )

    barrier = pltpu.get_barrier_semaphore()

    def greet(hot_to, cold_to):
        pl.semaphore_signal(
            barrier, inc=1, device_id=(hot_to, cold_to), device_id_type=MESH
        )

    other_x = (1 - x_hi) * 2 + 1
    for k in FAR_PLANE:
        greet(in_plane(in_plane_at(k)[0]), partner)
    for k in NEAR_Z:
        greet(along_z(ring(z, k)), partner)

    @pl.when(adds)
    def _():
        for k in (*FAR_PLANE, 0):
            greet(in_plane(in_plane_at(k)[0]), x_hi * 2)
        for k in NEAR_Z:
            greet(along_z(ring(z, k)), x_hi * 2)
        greet(hot, other_x)

    @pl.when(core == 0)
    def _():
        greet(hot, partner)

    landed(msk, load_sem.at[0])
    mpad[...] = jnp.zeros_like(mpad)
    mpad[0:blocks_here, 0:seqs] = msk[...]
    block_id = lax.broadcasted_iota(jnp.int32, mpad.shape, 0)
    lane_id = lax.broadcasted_iota(jnp.int32, mpad.shape, 1)
    active = jnp.broadcast_to(jnp.max(mpad[...], axis=1, keepdims=True), mpad.shape)
    upto = active
    step = 1
    while step < 32:
        upto = upto + jnp.where(block_id >= step, pltpu.roll(upto, step, 0), 0)
        step *= 2
    ahead = upto - active
    rank = jnp.where(active > 0, ahead, upto[31:32] + block_id - ahead)
    order = jnp.sum(jnp.where(rank == lane_id, block_id, 0), axis=0, keepdims=True)
    slots = [order[0, k] for k in range(CAP)]

    landed(tok, load_sem.at[1])
    landed(gain, load_sem.at[2])

    def add_squares(c, total):
        x = tok[:, place(c)].astype(F32)
        return total + x * x

    squares = lax.fori_loop(
        0, features // LANES, add_squares, jnp.zeros((seqs, LANES), F32), unroll=32
    )
    scale = lax.rsqrt(jnp.sum(squares, axis=1, keepdims=True) / features + EPS)
    mine = (tok[:, place(hot)].astype(F32) * scale * gain[:, place(hot)]).astype(BF16)

    landed(cgu, load_sem.at[3])
    start_loads(loads[5:])

    @pl.when(adds)
    def _():
        own_piece.start()

    for k in range(CAP):
        cols = pl.ds(slots[k] * LANES, LANES)
        both = jnp.concatenate([cgu[0, :, cols], cgu[1, :, cols]], axis=1)
        part = jnp.dot(mine, both, preferred_element_type=F32).astype(BF16)
        for r in range(4):
            at = 2 * r + k % 2
            s1[k // 2, at, 0] = part[16 * r : 16 * r + 16, :LANES]
            s1[k // 2, at, 1] = part[16 * r : 16 * r + 16, LANES:]

    @pl.when(adds)
    def _():
        pl.semaphore_wait(barrier, 24)
        for k in (2, 6):
            for core_to in range(2):
                pl.semaphore_signal(
                    zgo,
                    inc=1,
                    device_id=(along_z(ring(z, k)), x_hi * 2 + core_to),
                    device_id_type=MESH,
                )
        pl.semaphore_signal(xgo, inc=1, device_id=(hot, other_x), device_id_type=MESH)

    @pl.when(core == 0)
    def _():
        pl.semaphore_wait(barrier, 12)

    def plane_copies(order, op):
        for k in (*order, 0):
            to = in_plane_at(k)[0]
            sends = swap(core, to) < PAIRS
            if k == 0:
                sends = jnp.logical_and(sends, core == 0)
            op(k, to, sends)

    def s1_copy(k, to):
        return remote(
            s1.at[pair_of(core, to)],
            r1.at[core * RING + p],
            plane_send,
            s1_recv.at[core],
            in_plane(to),
            partner,
        )

    def start_s1(k, to, sends):
        @pl.when(sends)
        def _():
            s1_copy(k, to).start()

    plane_copies(FAR_PLANE, start_s1)

    def z_copies(order, op):
        for k in order:
            if k:
                op(k)
            else:
                pl.when(core == 0)(lambda: op(0))

    def hd_copy(k):
        to = ring(z, k)
        return remote(
            hd_hbm.at[:, columns_of(to)],
            hdp.at[core * RING + z],
            hd_send,
            hd_recv,
            along_z(to),
            partner,
        )

    z_copies((*NEAR_Z, 0), lambda k: hd_copy(k).start())

    half = lax.rem(z, 2)
    rows = lax.div(z, 2)
    slot_own = pair_of(core, p) * 2 + half
    block_own = jnp.int32(0)
    for k in range(CAP):
        block_own = jnp.where(slot_own == k, slots[k], block_own)
    landed(hidx, load_sem.at[5])
    unit = (cold * blocks_here + block_own) * LANES + lax.broadcasted_iota(
        jnp.int32, (LANES, LANES), 0
    )

    def match(c, found):
        return jnp.where(hidx[:, place(c)] == unit, 1.0, found)

    found = lax.fori_loop(
        0, hidx.shape[1] // LANES, match, jnp.zeros((LANES, LANES), F32), unroll=4
    )
    hot_units = lax.dot_general(
        jnp.ones((8, LANES), BF16),
        found.astype(BF16),
        (((1,), (1,)), ((), ())),
        preferred_element_type=F32,
    )[0:1]
    chosen = jnp.sum(
        jnp.where(block_id == block_own, mpad[...], 0).astype(F32), axis=0, keepdims=True
    )
    row = lax.broadcasted_iota(jnp.int32, (16, LANES), 0) + rows * 16
    column = lax.broadcasted_iota(jnp.int32, (16, LANES), 1)
    seq_live = jnp.sum(jnp.where(row == column, chosen, 0.0), axis=1, keepdims=True)
    lv[core] = (seq_live * (1.0 - jnp.minimum(hot_units, 1.0))).astype(BF16)
    lv_copy = remote(lv.at[0], lv.at[0], lv_send, lv_recv, hot, partner)

    @pl.when(core == 0)
    def _():
        lv_copy.start()

    landed(cd, load_sem.at[6])
    for k in range(CAP):
        block = cd[pl.ds(slots[k] * LANES, LANES), :]
        cds[k // 2, :, LANES * (k % 2) : LANES * (k % 2) + LANES] = jnp.transpose(block)

    pl.semaphore_wait(zgo, 2)
    z_copies(BEYOND_Z, lambda k: hd_copy(k).start())

    landed(hw, load_sem.at[4])

    def hot_chunk(c, total):
        cols = pl.ds(pl.multiple_of(c * CHUNK, CHUNK), CHUNK)
        normed = (tok[:, cols].astype(F32) * scale * gain[:, cols]).astype(BF16)
        return total + lax.dot_general(
            hw[:, cols], normed, (((1,), (1,)), ((), ())), preferred_element_type=F32
        )

    hot_t = lax.fori_loop(
        0, features // CHUNK, hot_chunk, jnp.zeros((32, seqs), F32)
    )
    hidden_t = silu(hot_t[:16]) * hot_t[16:]
    hh[core * RING + z] = jnp.concatenate([hidden_t, jnp.zeros_like(hidden_t)], axis=1).astype(
        BF16
    )

    def hh_copy(k):
        return remote(
            hh.at[core * RING + z],
            hh.at[core * RING + z],
            hh_send,
            hh_recv,
            along_z(ring(z, k)),
            partner,
        )

    z_copies((*FAR_Z, 0), lambda k: hh_copy(k).start())

    def cd_copy(k, to):
        return remote(
            cds.at[pair_of(core, to)],
            cdr.at[core, p],
            plane_send,
            cd_recv.at[core],
            in_plane(to),
            partner,
        )

    def start_cd(k, to, sends):
        @pl.when(sends)
        def _():
            cd_copy(k, to).start()

    def s2_copy(group, k):
        to = ring(z, k)
        return remote(
            s2.at[group, to],
            r2.at[group * RING + z],
            s2_send,
            r2_recv.at[group],
            along_z(to),
            partner,
        )

    piece = half * 4 + rows

    def h3_copy(group, to):
        return remote(
            h3.at[group, piece],
            h3.at[group, piece],
            h3_send,
            h3_recv.at[group],
            along_z(to),
            partner,
        )

    def fs_copy(to, x_to, core_to):
        dy = lax.rem(to // 2 + 4 - lax.div(p, 2), 4)
        dx = lax.rem(to + p, 2)
        dc = lax.rem(x_to + x_hi, 2)
        return remote(
            fs.at[4 * to + 2 * x_to + core_to],
            fr.at[2 * (2 * dy + dx) + dc],
            fs_send,
            fs_recv,
            in_plane(to),
            2 * x_to + core_to,
        )

    @pl.when(core == 0)
    def _():
        pl.semaphore_wait(go, 1)
        plane_copies(FAR_PLANE, start_cd)

    @pl.when(adds)
    def _():
        for group in (1, 0):

            @pl.when(works(group))
            def _():
                if group:
                    total = s1[pair_of(1, p)].astype(F32)
                else:
                    total = jnp.zeros(s1.shape[1:], F32)
                base = group * RING
                landed(r1.at[pl.ds(base, RING - group)], s1_recv.at[group])
                for k in range(group, RING):
                    total = total + r1[base + ring(p, k)].astype(F32)
                s2[group] = total.astype(BF16)
                for k in FAR_Z:
                    s2_copy(group, k).start()
                r2[base + z] = s2[group, z]

        pl.semaphore_signal(
            go, inc=1, device_id=(hot, x_hi * 2), device_id_type=MESH
        )

        plane_copies(FAR_PLANE, start_cd)
        cdr[1, p] = cds[pair_of(1, p)]

        remote(lv.at[0], lv.at[0], lv_send, lv_recv, hot, partner).wait_recv()
        for group in (1, 0):

            @pl.when(works(group))
            def _():
                pieces = r2.at[pl.ds(group * RING, RING)]
                landed(pieces.at[pl.ds(0, RING - 1)], r2_recv.at[group])
                both = pieces[0].astype(F32)
                for i in range(1, RING):
                    both = both + pieces[i].astype(F32)
                live = lv[group].astype(F32)
                h3[group, piece] = (silu(both[0]) * both[1] * live).astype(BF16)
                for to in range(RING):
                    pl.when(to != z)(h3_copy(group, to).start)

        own_piece.wait()
        landed(hdp.at[pl.ds(0, 2 * RING - 1)], hd_recv)
        landed(hh.at[pl.ds(0, 2 * RING - 1)], hh_recv)
        hidden = hh[...].reshape(2 * LANES, LANES)[:, :seqs]
        for q in range(RING):
            down = hdp[:, :, LANES * q : LANES * q + LANES].reshape(2 * LANES, LANES)
            acc[q] = jnp.dot(jnp.transpose(down), hidden, preferred_element_type=F32)

        pl.semaphore_wait(xgo, 1)

        def await_pair(group):
            @pl.when(works(group))
            def _():
                landed(cdr.at[group, pl.ds(0, RING - group)], cd_recv.at[group])
                landed(h3.at[group, pl.ds(0, RING - 1)], h3_recv.at[group])

        def pair_hidden(group):
            return jnp.concatenate(
                [
                    h3[group, 0:4].reshape(seqs, LANES),
                    h3[group, 4:8].reshape(seqs, LANES),
                ],
                axis=1,
            )

        def pair_term(group, values, to):
            term = lax.dot_general(
                cdr[group, to],
                values,
                (((1,), (1,)), ((), ())),
                preferred_element_type=F32,
            )
            return acc[to] + jnp.where(works(group), term, 0.0)

        await_pair(1)
        values = pair_hidden(1)
        for q in range(RING):
            acc[q] = pair_term(1, values, q)
        await_pair(0)

        values = pair_hidden(0)
        terms = [pair_term(0, values, to) for to in range(RING)]
        for to, term in enumerate(terms):
            for c in range(4):
                fs[4 * to + c] = jnp.concatenate(
                    [term[32 * c : 32 * c + 16], term[32 * c + 16 : 32 * c + 32]], axis=1
                ).astype(BF16)
            for x_to, core_to in ((0, 1), (0, 0), (1, 1), (1, 0)):
                copy = fs_copy(to, x_to, core_to)
                if core_to:
                    own = jnp.logical_and(to == p, x_hi == x_to)
                    pl.when(jnp.logical_not(own))(copy.start)
                else:
                    copy.start()

        fr[0] = fs[4 * p + cold]

    @pl.when(adds)
    def _():
        landed = fr.at[pl.ds(1, 2 * RING - 1)]
        pltpu.make_async_copy(landed, landed, fs_recv).wait()

    @pl.when(core == 0)
    def _():
        pltpu.make_async_copy(fr, fr, fs_recv).wait()

    result = fr[0].astype(F32)
    for i in range(1, 2 * RING):
        result = result + fr[i].astype(F32)
    out_ref[0:16, :] = result[:, :seqs].astype(BF16)
    out_ref[16:32, :] = result[:, seqs:].astype(BF16)

    fewer = jnp.logical_and(adds, works(1))

    @pl.when(fewer)
    def _():
        landed(r1.at[pl.ds(0, 2 * PAIRS - 2)], plane_send)

    @pl.when(jnp.logical_not(fewer))
    def _():
        landed(r1.at[pl.ds(0, 2 * PAIRS)], plane_send)

    @pl.when(core == 0)
    def _():
        landed(hdp.at[pl.ds(0, RING)], hd_send)
        landed(hh.at[pl.ds(0, RING)], hh_send)
        lv_copy.wait_send()

    @pl.when(adds)
    def _():
        landed(hdp.at[pl.ds(0, RING - 1)], hd_send)
        landed(hh.at[pl.ds(0, RING - 1)], hh_send)
        landed(fs.at[pl.ds(0, 4 * RING - 1)], fs_send)
        both_groups = jnp.logical_and(works(0), works(1))

        @pl.when(both_groups)
        def _():
            landed(r2.at[pl.ds(0, 2 * RING - 2)], s2_send)
            landed(hh.at[pl.ds(0, 2 * RING - 2)], h3_send)

        @pl.when(jnp.logical_not(both_groups))
        def _():
            landed(r2.at[pl.ds(0, RING - 1)], s2_send)
            landed(hh.at[pl.ds(0, RING - 1)], h3_send)


def on_device(
    tokens,
    norm_gain,
    hot_gate,
    hot_up,
    hot_down,
    hot_index,
    cold_gate,
    cold_up,
    cold_down,
    block_mask,
):
    seqs, features = tokens.shape
    dma = pltpu.SemaphoreType.DMA
    any_space = pl.BlockSpec(memory_space=pl.ANY)
    return pl.pallas_call(
        kernel,
        out_shape=jax.ShapeDtypeStruct((32, seqs), BF16),
        in_specs=[any_space] * 10,
        out_specs=pl.BlockSpec(memory_space=pltpu.VMEM),
        scratch_shapes=[
            pltpu.VMEM(tokens.shape, BF16),
            pltpu.VMEM((1, features), F32),
            pltpu.VMEM((32, features), BF16),
            pltpu.VMEM((1, hot_index.shape[0]), jnp.int32),
            pltpu.VMEM((2, *cold_gate.shape), BF16),
            pltpu.VMEM(cold_down.shape, BF16),
            pltpu.VMEM(block_mask.shape[::-1], jnp.int32),
            pltpu.VMEM((32, LANES), jnp.int32),
            pltpu.VMEM((PAIRS, RING, 2, 16, LANES), BF16),
            pltpu.VMEM((2 * RING, RING, 2, 16, LANES), BF16),
            pltpu.VMEM((2, RING, 2, 16, LANES), BF16),
            pltpu.VMEM((2 * RING, 2, 16, LANES), BF16),
            pltpu.VMEM((2, RING, 16, LANES), BF16),
            pltpu.VMEM((PAIRS, LANES, 2 * LANES), BF16),
            pltpu.VMEM((2, RING, LANES, 2 * LANES), BF16),
            pltpu.VMEM((2 * RING, 16, RING * LANES), BF16),
            pltpu.VMEM((2 * RING, 16, LANES), BF16),
            pltpu.VMEM((2, 16, LANES), BF16),
            pltpu.VMEM((RING, LANES, seqs), F32),
            pltpu.VMEM((RING * 4, 16, LANES), BF16),
            pltpu.VMEM((2 * RING, 16, LANES), BF16),
            dma((8,)),
            dma,
            dma((2,)),
            dma,
            dma((2,)),
            dma,
            dma((2,)),
            dma((2,)),
            dma,
            dma,
            dma,
            dma,
            dma,
            dma,
            pltpu.SemaphoreType.REGULAR,
            pltpu.SemaphoreType.REGULAR,
            pltpu.SemaphoreType.REGULAR,
            dma,
            dma,
        ],
        compiler_params=pltpu.CompilerParams(
            collective_id=0, has_side_effects=True, vmem_limit_bytes=55218 * 1024
        ),
    )(
        tokens,
        norm_gain.reshape(1, -1),
        hot_gate,
        hot_up,
        hot_down,
        hot_index.reshape(1, -1),
        cold_gate,
        cold_up,
        cold_down,
        block_mask.T,
    ).T


def solution(mesh):
    rows = P(("hot", "cold"), None)
    return jax.shard_map(
        on_device,
        mesh=mesh,
        in_specs=(
            P(),
            P(),
            rows,
            rows,
            rows,
            P(),
            P("hot", "cold"),
            P("hot", "cold"),
            P("cold", "hot"),
            P(None, "cold"),
        ),
        out_specs=P(None, ("hot", "cold")),
        check_vma=False,
    )
```
